32 devices in a mesh: atom: 4 (over x, core), aux: 8 (over z, y).
Axes of the slice: x: 2, y: 2, z: 4, core: 2. Of those that a mesh axis runs over, the one named last changes fastest.
Arguments:
- three_index: bfloat16 [256, 8, 4, 128, 128], P('aux', 'atom'), may hold values from -0.09375 to 0.09375
- density: bfloat16 [1024, 1024], P(('atom', 'aux')), may hold values from -6 to 6
- pair_blocks: int32 [8, 4], replicated, may hold values from 0 to 7, as said below
- basis_counts: int32 [8], replicated, may hold values from 1 to 128, 768 in all
Outputs:
- exchange_matrix: float32 [1024, 1024], P(('atom', 'aux'))
The draws below stay inside these ranges and needn't reach their ends.
Inputs may be any that keep to these rules, and one draw needn't show every extreme that they name: `pair_blocks`: each row names 4 different basis blocks, the first being the row's own block.
All inputs are finite; a program needn't handle non-finite values.
Results may differ from the reference program's by a relative error of at most 0.0029.
Values may be sent and summed in bfloat16 or wider, within the bound.
A program may use at most 192 MiB of HBM per device.

```python
import math
import jax
import jax.numpy as jnp
import numpy as np
from jax import lax

BS = 128
NAB = 1
NEIGH = 4
NBLK = 8
NBF = 1024
AUXW = 256


def draw_pair_blocks(key, part):
    scores = jax.random.randint(key, (NBLK, NBLK), 0, 1 << 20)
    indices = jnp.arange(NBLK)
    scores = scores * NBLK + indices[None, :]
    scores = jnp.where(indices[:, None] == indices[None, :], -1, scores)
    ordering = jnp.argsort(scores, axis=1, stable=True)
    return ordering[:, :NEIGH].astype(jnp.int32)


def shard_levels(rng, dims, shards, smallest, largest):
    factor_of = 1.0
    for position, parts in shards:
        steps = jax.random.uniform(jax.random.fold_in(jax.random.fold_in(rng, 6), position), (parts,), jnp.float32, smallest / len(shards), largest / len(shards))
        factor_of = factor_of * jnp.repeat(jnp.exp(steps), dims[position] // parts).reshape((-1,) + (1,) * (len(dims) - 1 - position))
    return factor_of


def split_up(number_of, total, reach, slope):
    portions = [(1 << 20) // math.isqrt(rank ** slope) + 1 for rank in range(2, number_of + 1)]
    surplus, holding = total - reach - (number_of - 1), [1] * (number_of - 1)
    while surplus > 0:
        free = [i for i in range(number_of - 1) if holding[i] < reach]
        whole, remaining = sum([portions[i] for i in free]), surplus
        for i in free:
            more = min(reach - holding[i], max(1, remaining * portions[i] // whole), surplus)
            holding[i] = holding[i] + more
            surplus = surplus - more
    return np.array([reach] + holding)


def ragged(rng, amount, total, bound, slope):
    if amount == 2:
        one = jax.random.randint(rng, (), max(1, total - bound), min(bound, total - 1) + 1)
        return jnp.stack([one, total - one])
    lengths = jnp.asarray(split_up(amount, total, bound, slope), jnp.int32)
    couples = (amount - 1) // 2
    donor, receiver = lengths[1:1 + 2 * couples:2], lengths[2:2 + 2 * couples:2]
    slack = jnp.minimum(donor - 1, bound - receiver)
    shifted = jax.random.randint(jax.random.fold_in(rng, 1), (couples,), 0, 1 << 20) % (slack + 1)
    lengths = lengths.at[1:1 + 2 * couples:2].set(donor - shifted).at[2:2 + 2 * couples:2].set(receiver + shifted)
    return lengths[jax.random.permutation(jax.random.fold_in(rng, 2), amount)]


def gaussian(own_key, extent, width, reach, shards=(), kind=jnp.bfloat16):
    loudness = shard_levels(own_key, extent, shards, -0.22, 0.18) if shards else 1.0
    array = jax.random.normal(own_key, extent, jnp.float32) * width * loudness
    return jnp.minimum(jnp.maximum(array, -reach), reach).astype(kind)


def setup_inputs(seed: int = 0) -> dict:
    keys = jax.random.split(jax.random.key(seed), 5)
    return {
        "three_index": gaussian(keys[0], (AUXW, NBLK, NEIGH, BS, BS), (NEIGH * BS * 8 * NAB) ** -0.5, 0.09375, ((0, 8), (1, 4))),
        "density": gaussian(keys[1], (NBF, NBF), 1.0, 6.0, ((0, 32),)),
        "pair_blocks": draw_pair_blocks(jax.random.fold_in(keys[4], 71), 0),
        "basis_counts": ragged(keys[3], NBLK, NBLK * BS * 3 // 4, BS, 2).astype(jnp.int32),
    }


def reference(three_index, density, pair_blocks, basis_counts):
    live_slots = (jnp.arange(BS)[None, :] < basis_counts[:, None]).astype(jnp.bfloat16)
    col_live = live_slots[pair_blocks]
    masked = three_index * live_slots[None, :, None, :, None] * col_live[None, :, :, None, :]
    near_density = density.reshape(NBLK, BS, NBF)[pair_blocks]
    placement = (pair_blocks.reshape(-1)[:, None] == jnp.arange(NBLK)[None, :]).astype(jnp.float32)
    group_size = math.gcd(AUXW, 8)
    grouped = masked.reshape(AUXW // group_size, group_size, NBLK, NEIGH, BS, BS)

    def advance(running, portion):
        halfway = jnp.einsum('pmjab,mjbs->pmas', portion.astype(jnp.float32), near_density.astype(jnp.float32))
        halfway = halfway.astype(jnp.bfloat16).reshape(group_size, NBF, NBLK, BS)
        contrib = jnp.einsum('pmbc,pbjcn->mbjn', halfway.astype(jnp.float32), portion.astype(jnp.float32))
        spread_out = jnp.einsum('mqn,qk->mkn', contrib.reshape(NBF, NBLK * NEIGH, BS), placement,
                                precision=lax.Precision.HIGHEST)
        return running + spread_out.reshape(NBF, NBF), None

    running, _ = lax.scan(advance, jnp.zeros((NBF, NBF), jnp.float32), grouped)
    return running
```

```python
import functools
import math

import jax
import jax.numpy as jnp
from jax import lax
from jax.experimental import pallas as pl
from jax.experimental.pallas import tpu as pltpu
from jax.sharding import PartitionSpec as P

MESH = pl.DeviceIdType.MESH


def kernel(
    atoms, aux, xs, ys, zs,
    pair_hbm, counts_hbm, tensor_ref, piece_ref, out_ref,
    pair_ref, counts_ref, dens, tens, wide, half, send, total, from_core,
    first_x, first_y, first_z, second_y, second_x, second_z,
    own_sem, piece_sem, pair_sem, counts_sem, t_send, t_recv, d_send, d_recv, k_send, k_recv,
):
    per, nblk, neigh, bs = tens.shape[0], tens.shape[1], tens.shape[2], tens.shape[3]
    nbf = total.shape[1]
    own_blocks = nblk // atoms
    rows = piece_ref.shape[0]
    group = aux * rows
    t = lax.axis_index("atom")
    u = lax.axis_index("aux")
    x, c = t // 2, t % 2
    z, y = u // ys, u % ys

    pair_copy = pltpu.make_async_copy(pair_hbm, pair_ref, pair_sem)
    counts_copy = pltpu.make_async_copy(counts_hbm, counts_ref, counts_sem)
    pair_copy.start()
    counts_copy.start()

    def atom_peer(d):
        return lax.rem(t + d, atoms)

    def x_peer(e):
        return lax.rem(x + e, xs) * 2 + c

    def y_peer(e):
        return z * ys + lax.rem(y + e, ys)

    def z_peer(e):
        return lax.rem(z + e, zs) * ys + y

    barrier = pltpu.get_barrier_semaphore()
    for d in range(1, atoms):
        pl.semaphore_signal(barrier, inc=1, device_id=(atom_peer(d), u), device_id_type=MESH)
    for e in range(1, ys):
        pl.semaphore_signal(barrier, inc=1, device_id=(t, y_peer(e)), device_id_type=MESH)
    for e in range(1, zs):
        pl.semaphore_signal(barrier, inc=1, device_id=(t, z_peer(e)), device_id_type=MESH)
    pl.semaphore_wait(barrier, (atoms - 1) + (ys - 1) + (zs - 1))

    counter = [0]

    def remote(src, dst, device, sems):
        k = counter[0]
        counter[0] += 1
        return pltpu.make_async_remote_copy(
            src_ref=src, dst_ref=dst, send_sem=sems[0].at[k], recv_sem=sems[1].at[k],
            device_id=device, device_id_type=MESH,
        )

    dsems = (d_send, d_recv)

    def dens_rows(first, count):
        return dens.at[first // bs, pl.ds(pl.multiple_of(first % bs, 16), count), :]

    mine = (t * aux + u) * rows
    local = pltpu.make_async_copy(piece_ref, dens_rows(mine, rows), piece_sem)
    local.start()
    over_x = []
    for e in range(1, xs):
        cp = remote(piece_ref, dens_rows(mine, rows), (x_peer(e), u), dsems)
        cp.start()
        over_x.append(cp)

    def own_copy(i):
        return pltpu.make_async_copy(
            tensor_ref.at[t * per + i], tens.at[i, pl.ds(t * own_blocks, own_blocks)], own_sem.at[i]
        )

    def t_copy(i, d):
        to = atom_peer(d)
        return pltpu.make_async_remote_copy(
            src_ref=tensor_ref.at[to * per + i],
            dst_ref=tens.at[i, pl.ds(t * own_blocks, own_blocks)],
            send_sem=t_send.at[i, d - 1],
            recv_sem=t_recv.at[i, d - 1],
            device_id=(to, u),
            device_id_type=MESH,
        )

    order = list(range(1, atoms, 2)) + list(range(2, atoms, 2))

    def begin(i, carry):
        for d in order:
            t_copy(i, d).start()
        own_copy(i).start()
        return carry

    lax.fori_loop(0, per, begin, 0)

    local.wait()
    for cp in over_x:
        cp.wait()
    over_y = []
    for xx in range(xs):
        first = ((xx * 2 + c) * aux + u) * rows
        for e in range(1, ys):
            cp = remote(dens_rows(first, rows), dens_rows(first, rows), (t, y_peer(e)), dsems)
            cp.start()
            over_y.append(cp)
    total[...] = jnp.zeros_like(total)
    for cp in over_y:
        cp.wait()
    over_z = []
    for xx in range(xs):
        first = ((xx * 2 + c) * aux + z * ys) * rows
        for e in range(1, zs):
            cp = remote(dens_rows(first, ys * rows), dens_rows(first, ys * rows), (t, z_peer(e)), dsems)
            cp.start()
            over_z.append(cp)
    for cp in over_z:
        cp.wait()
    over_c = []
    for xx in range(xs):
        blocks = dens.at[pl.ds((xx * 2 + c) * own_blocks, own_blocks)]
        cp = remote(blocks, blocks, (x * 2 + (1 - c), u), dsems)
        cp.start()
        over_c.append(cp)
    for cp in over_c:
        cp.wait()

    pair_copy.wait()
    counts_copy.wait()
    lane = lax.broadcasted_iota(jnp.int32, (1, bs), 1)
    col_live = jnp.concatenate(
        [jnp.where(lane < counts_ref[b], 1.0, 0.0).astype(jnp.float32) for b in range(nblk)], axis=1
    )

    def mask_rows(b, carry):
        slot = lax.broadcasted_iota(jnp.int32, (bs, 1), 0)
        row_live = jnp.where(slot < counts_ref[b], 1.0, 0.0).astype(jnp.float32)
        dens[b] = (dens[b].astype(jnp.float32) * row_live * col_live).astype(dens.dtype)
        return carry

    lax.fori_loop(0, nblk, mask_rows, 0)

    side = nbf // 2
    cols = min(side, 512)

    def at_rows(first, count):
        return pl.ds(pl.multiple_of(first, 16), count)

    def arrive(i):
        own_copy(i).wait()
        for d in range(1, atoms):
            t_copy(i, d).wait_recv()

    def first_half(i, first, count):
        def block_row(k, carry):
            m = first + k
            left = jnp.concatenate([tens[i, m, j] for j in range(neigh)], axis=1)
            right = jnp.concatenate([dens[pair_ref[j, m]] for j in range(neigh)], axis=0)
            h = jnp.dot(left, right, preferred_element_type=jnp.float32)
            at = pl.ds(pl.multiple_of(m * bs, bs), bs)
            half[at, :] = h.astype(half.dtype)
            for n in range(nblk):
                block = jnp.zeros((bs, bs), wide.dtype)
                for j in range(neigh):
                    block = jnp.where(pair_ref[j, m] == n, tens[i, m, j], block)
                wide[at, n * bs:(n + 1) * bs] = block
            return carry

        lax.fori_loop(0, count, block_row, 0)

    def product(g, h):
        at = at_rows(g * group, group)
        for k in range(side // cols):
            lo = h * side + k * cols
            total[at, lo:lo + cols] += jnp.dot(
                half[at, :], wide[:, lo:lo + cols], preferred_element_type=jnp.float32
            )

    def one(i, carry):
        arrive(i)
        first_half(i, 0, nblk)

        def second_half(g, carry):
            product(g, 0)
            product(g, 1)
            return carry

        lax.fori_loop(0, atoms, second_half, 0)
        return carry

    lax.fori_loop(0, per - 1, one, 0)

    counter[0] = 0
    ksems = (k_send, k_recv)
    sends = []

    def send_to(src, dst, device):
        cp = remote(src, dst, device, ksems)
        cp.start()
        sends.append(cp)
        return cp

    other = 1 - c
    sibling = (x * 2 + other, u)
    final = per - 1
    own_copy(final).wait()
    for d in order[:-1]:
        t_copy(final, d).wait_recv()
    late = lax.rem(t + atoms - order[-1], atoms)

    def part_product(g, q, h):
        at, qt = at_rows(g * group, group), at_rows(q * group, group)
        qc = pl.ds(pl.multiple_of(q * group, 128), group)
        for k in range(side // cols):
            lo = h * side + k * cols
            total[at, lo:lo + cols] += jnp.dot(
                half[at, qc], wide[qt, lo:lo + cols], preferred_element_type=jnp.float32
            )

    def early_rows(k, carry):
        first_half(final, lax.rem(late + k, atoms) * own_blocks, own_blocks)
        return carry

    lax.fori_loop(1, atoms, early_rows, 0)

    def early_products(k, carry):
        g = (k // (atoms - 1)) * 2 + other
        q = lax.rem(late + 1 + k % (atoms - 1), atoms)
        part_product(g, q, 0)
        part_product(g, q, 1)
        return carry

    lax.fori_loop(0, xs * (atoms - 1), early_products, 0)
    t_copy(final, order[-1]).wait_recv()
    first_half(final, late * own_blocks, own_blocks)

    def last_product(e, core, h):
        if core is c:
            product(x_at(e) * 2 + c, h)
        else:
            part_product(x_at(e) * 2 + other, late, h)

    left, right = slice(0, side), slice(side, nbf)

    def x_at(e):
        return lax.rem(x + e, xs)

    def y_at(e):
        return lax.rem(y + e, ys)

    core_left, core_right = {}, {}
    for e in list(range(1, xs)) + [0]:
        last_product(e, other, 0)
        last_product(e, other, 1)
        for store, part in ((core_left, left), (core_right, right)):
            store[e] = send_to(
                total.at[at_rows((x_at(e) * 2 + other) * group, group), part],
                from_core.at[e * group:(e + 1) * group, part],
                sibling,
            )

    def core_sum(e, row, count, part):
        return (
            total[at_rows((x_at(e) * 2 + c) * group + row, count), part]
            + from_core[at_rows(e * group + row, count), part]
        )

    zr = zs * rows
    left_x = {}
    for e in range(1, xs):
        last_product(e, c, 0)
        core_left[e].wait_recv()
        for f in list(range(1, ys)) + [0]:
            lo = (e - 1) * group + f * zr
            for zz in range(zs):
                send[lo + zz * rows:lo + (zz + 1) * rows, left] = core_sum(
                    e, (zz * ys + y_at(f)) * rows, rows, left
                ).astype(send.dtype)
            left_x[e, f] = send_to(
                send.at[lo:lo + zr, left], first_x.at[lo:lo + zr, :], (x_at(e) * 2 + c, u)
            )
    right_y = {}
    for e in list(range(1, xs)) + [0]:
        last_product(e, c, 1)
        core_right[e].wait_recv()
        for f in range(1, ys):
            lo = ((f - 1) * xs + e) * zr
            to = (f - 1) * xs * zr + x_at(e) * zr
            for zz in range(zs):
                send[lo + zz * rows:lo + (zz + 1) * rows, right] = core_sum(
                    e, (zz * ys + y_at(f)) * rows, rows, right
                ).astype(send.dtype)
            right_y[f, e] = send_to(
                send.at[lo:lo + zr, right], second_y.at[at_rows(to, zr), :], (t, y_peer(f))
            )
    last_product(0, c, 0)
    core_left[0].wait_recv()

    def left_after_x(zz, f):
        value = core_sum(0, (zz * ys + y_at(f)) * rows, rows, left)
        for e in range(xs - 1):
            row = e * group + f * zr + zz * rows
            value = value + first_x[at_rows(row, rows), :].astype(jnp.float32)
        return value

    stage = max((xs - 1) * group, (ys - 1) * xs * zr)
    left_y = []
    for f in range(1, ys):
        lo = stage + (f - 1) * zr
        for e in range(1, xs):
            left_x[e, f].wait_recv()
        for zz in range(zs):
            send[lo + zz * rows:lo + (zz + 1) * rows, left] = left_after_x(zz, f).astype(send.dtype)
        left_y.append(send_to(
            send.at[lo:lo + zr, left], first_y.at[(f - 1) * zr:f * zr, :], (t, y_peer(f))
        ))

    def right_after_y(e, zz):
        value = core_sum(e, (zz * ys + y) * rows, rows, right)
        for f in range(ys - 1):
            row = f * xs * zr + x_at(e) * zr + zz * rows
            value = value + second_y[at_rows(row, rows), :].astype(jnp.float32)
        return value

    right_x = []
    for e in range(1, xs):
        lo = stage + (e - 1) * zr
        for f in range(1, ys):
            right_y[f, e].wait_recv()
        for zz in range(zs):
            send[lo + zz * rows:lo + (zz + 1) * rows, right] = right_after_y(e, zz).astype(send.dtype)
        right_x.append(send_to(
            send.at[lo:lo + zr, right], second_x.at[(e - 1) * zr:e * zr, :], (x_at(e) * 2 + c, u)
        ))

    def left_after_y(zz):
        value = left_after_x(zz, 0)
        for f in range(ys - 1):
            value = value + first_y[at_rows(f * zr + zz * rows, rows), :].astype(jnp.float32)
        return value

    def right_after_x(zz):
        value = right_after_y(0, zz)
        for e in range(xs - 1):
            value = value + second_x[at_rows(e * zr + zz * rows, rows), :].astype(jnp.float32)
        return value

    stage = stage + max(xs - 1, ys - 1) * zr
    ends = []
    for waits, after, into, part in (
        (left_y, left_after_y, first_z, left), (right_x, right_after_x, second_z, right)
    ):
        for cp in waits:
            cp.wait_recv()
        if part == right:
            for f in range(1, ys):
                right_y[f, 0].wait_recv()
        else:
            for e in range(1, xs):
                left_x[e, 0].wait_recv()
        arrivals = []
        for e in range(1, zs):
            lo = stage + (e - 1) * rows
            send[lo:lo + rows, part] = after(lax.rem(z + e, zs)).astype(send.dtype)
            arrivals.append(send_to(
                send.at[lo:lo + rows, part], into.at[(e - 1) * rows:e * rows, :], (t, z_peer(e))
            ))
        ends.append((arrivals, after, into, part))
    block = mine // bs
    slot = lax.broadcasted_iota(jnp.int32, (rows, 1), 0) + mine % bs
    row_live = jnp.where(slot < counts_ref[block], 1.0, 0.0).astype(jnp.float32)
    for arrivals, after, into, part in ends:
        value = after(z)
        for e in range(zs - 1):
            arrivals[e].wait_recv()
            value = value + into[e * rows:(e + 1) * rows, :].astype(jnp.float32)
        out_ref[:, part] = value * row_live * col_live[:, part]
    for cp in sends:
        cp.wait_send()

    def finish(i, carry):
        for d in range(1, atoms):
            t_copy(i, d).wait_send()
        return carry

    lax.fori_loop(0, per, finish, 0)


def plain_device(atoms, aux, three_index, density, pair_blocks, basis_counts):
    aux_here, own_blocks, neigh, bs, _ = three_index.shape
    rows, nbf = density.shape
    nblk = nbf // bs
    xs = atoms // 2
    ys = xs if aux % xs == 0 else 1
    zs = aux // ys
    per = aux_here // atoms
    group = aux * rows
    n_d = (xs - 1) + xs * (ys - 1) + xs * (zs - 1) + xs
    n_k = 2 * (xs + (xs - 1) + (ys - 1) + (zs - 1)) + 2 * (xs - 1) * (ys - 1)
    side = nbf // 2
    zr = zs * rows
    send_rows = max((xs - 1) * group, (ys - 1) * xs * zr) + max(xs - 1, ys - 1) * zr + zr
    vmem, dma = pltpu.VMEM, pltpu.SemaphoreType.DMA
    bf16, f32 = jnp.bfloat16, jnp.float32
    return pl.pallas_call(
        functools.partial(kernel, atoms, aux, xs, ys, zs),
        out_shape=jax.ShapeDtypeStruct((rows, nbf), f32),
        in_specs=[
            pl.BlockSpec(memory_space=pl.ANY),
            pl.BlockSpec(memory_space=pl.ANY),
            pl.BlockSpec(memory_space=pl.ANY),
            pl.BlockSpec(memory_space=pl.ANY),
        ],
        out_specs=pl.BlockSpec(memory_space=pltpu.VMEM),
        scratch_shapes=[
            pltpu.SMEM(pair_blocks.shape[::-1], jnp.int32),
            pltpu.SMEM(basis_counts.shape, jnp.int32),
            vmem((nblk, bs, nbf), bf16),
            vmem((per, nblk, neigh, bs, bs), bf16),
            vmem((nbf, nbf), bf16),
            vmem((nbf, nbf), bf16),
            vmem((send_rows, nbf), bf16),
            vmem((nbf, nbf), f32),
            vmem((xs * group, nbf), f32),
            vmem((max(xs - 1, 1) * group, side), bf16),
            vmem((max(ys - 1, 1) * zs * rows, side), bf16),
            vmem((max(zs - 1, 1) * rows, side), bf16),
            vmem((max(ys - 1, 1) * xs * zs * rows, side), bf16),
            vmem((max(xs - 1, 1) * zs * rows, side), bf16),
            vmem((max(zs - 1, 1) * rows, side), bf16),
            dma((per,)),
            dma,
            dma,
            dma,
            dma((per, atoms - 1)),
            dma((per, atoms - 1)),
            dma((n_d,)),
            dma((n_d,)),
            dma((n_k,)),
            dma((n_k,)),
        ],
        compiler_params=pltpu.CompilerParams(
            collective_id=0, has_side_effects=True, vmem_limit_bytes=67043328
        ),
    )(pair_blocks.T, basis_counts, three_index, density)


def packed_kernel(
    cap, atoms, aux, xs, ys, zs,
    pair_hbm, counts_hbm, tensor_ref, piece_ref, out_ref,
    pair_ref, counts_ref, tiles_ref, width_ref, base_ref, take_ref, give_ref, which_ref,
    dens, raw, direct, outbox, inbox, stage, arrived, tens, pack, unpack,
    wide, half, send, total, from_core,
    first_x, first_y, first_z, second_y, second_x, second_z,
    own_sem, piece_sem, pair_sem, counts_sem, t_send, t_recv, p_send, p_recv, x_send, x_recv, dx_send, dx_recv, dz_send, dz_recv, dy_send, dy_recv,
    dc_send, dc_recv, k_send, k_recv,
):
    per, chip_blocks, neigh, bs = raw.shape[1], raw.shape[2], raw.shape[3], raw.shape[4]
    nbf = total.shape[1]
    nblk = nbf // bs
    own_blocks = nblk // atoms
    rows = piece_ref.shape[0]
    group = aux * rows
    tall = bs // 16
    span = neigh * bs
    slots = neigh + 1
    t = lax.axis_index("atom")
    u = lax.axis_index("aux")
    x, c = t // 2, t % 2
    z, y = u // ys, u % ys
    other = 1 - c
    sibling = (x * 2 + other, u)

    pair_copy = pltpu.make_async_copy(pair_hbm, pair_ref, pair_sem)
    counts_copy = pltpu.make_async_copy(counts_hbm, counts_ref, counts_sem)
    pair_copy.start()
    counts_copy.start()

    def x_at(e):
        return lax.rem(x + e, xs)

    def x_peer(e):
        return x_at(e) * 2 + c

    def y_peer(e):
        return z * ys + lax.rem(y + e, ys)

    def z_peer(e):
        return lax.rem(z + e, zs) * ys + y

    def own_copy(e, i):
        return pltpu.make_async_copy(
            tensor_ref.at[x_peer(e) * per + i], raw.at[e, i, pl.ds(c * own_blocks, own_blocks)], own_sem.at[e, i]
        )

    def core_copy(e, i):
        return pltpu.make_async_remote_copy(
            src_ref=tensor_ref.at[(x_at(e) * 2 + other) * per + i],
            dst_ref=raw.at[e, i, pl.ds(c * own_blocks, own_blocks)],
            send_sem=t_send.at[e, i], recv_sem=t_recv.at[e, i],
            device_id=sibling, device_id_type=MESH,
        )

    def x_copy(e, i):
        return pltpu.make_async_remote_copy(
            src_ref=outbox.at[e - 1, i], dst_ref=inbox.at[xs - e - 1, i],
            send_sem=x_send.at[e - 1, i], recv_sem=x_recv.at[xs - e - 1, i],
            device_id=(x_peer(e), u), device_id_type=MESH,
        )

    def plain_copy(e, core):
        return pltpu.make_async_remote_copy(
            src_ref=tensor_ref.at[(x_at(e) * 2 + core) * per],
            dst_ref=direct.at[xs - e - 1, pl.ds(c * own_blocks, own_blocks)],
            send_sem=p_send.at[e - 1, core], recv_sem=p_recv.at[xs - e - 1, c],
            device_id=(x_at(e) * 2 + core, u), device_id_type=MESH,
        )

    def plain_arrival(r, core):
        here = direct.at[r, pl.ds(core * own_blocks, own_blocks)]
        return pltpu.make_async_remote_copy(
            src_ref=here, dst_ref=here, send_sem=p_send.at[r, core], recv_sem=p_recv.at[r, core],
            device_id=sibling, device_id_type=MESH,
        )

    def piece(xx, zz, yy):
        first = ((xx * 2 + c) * aux + zz * ys + yy) * rows
        return dens.at[first // bs, pl.ds(pl.multiple_of(first % bs, 16), rows), :]

    def dens_copy(xx, zz, yy, device, send_sem, recv_sem):
        return pltpu.make_async_remote_copy(
            src_ref=piece(xx, zz, yy), dst_ref=piece(xx, zz, yy), send_sem=send_sem, recv_sem=recv_sem,
            device_id=device, device_id_type=MESH,
        )

    def dens_x(e):
        return pltpu.make_async_remote_copy(
            src_ref=piece_ref, dst_ref=piece(x, z, y), send_sem=dx_send.at[e - 1], recv_sem=dx_recv.at[e - 1],
            device_id=(x_peer(e), u), device_id_type=MESH,
        )

    def dens_z(up, xx, zz):
        to = (z + 1 if up else z - 1) * ys + y
        return dens_copy(xx, zz, y, (t, to), dz_send.at[int(up), zz, xx], dz_recv.at[zz, xx])

    def dens_y(e, xx, zz):
        return dens_copy(xx, zz, y, (t, y_peer(e)), dy_send.at[zz, xx, e - 1], dy_recv.at[zz, xx, e - 1])

    def dens_c(xx, zz, yy):
        return dens_copy(xx, zz, yy, sibling, dc_send.at[zz, yy, xx], dc_recv.at[zz, yy, xx])

    mine = (t * aux + u) * rows
    barrier = pltpu.get_barrier_semaphore()
    pl.semaphore_signal(barrier, inc=1, device_id=sibling, device_id_type=MESH)
    for e in range(1, xs):
        pl.semaphore_signal(barrier, inc=1, device_id=(x_peer(e), u), device_id_type=MESH)
        pl.semaphore_signal(barrier, inc=1, device_id=(x_at(e) * 2 + other, u), device_id_type=MESH)
    for e in range(1, ys):
        pl.semaphore_signal(barrier, inc=1, device_id=(t, y_peer(e)), device_id_type=MESH)
    for e in range(1, zs):
        pl.semaphore_signal(barrier, inc=1, device_id=(t, z_peer(e)), device_id_type=MESH)
    local = pltpu.make_async_copy(piece_ref, piece(x, z, y), piece_sem)
    local.start()
    pl.semaphore_wait(barrier, 1 + 2 * (xs - 1) + (ys - 1) + (zs - 1))

    for e in range(1, xs):
        dens_x(e).start()
    for e in range(1, xs):
        plain_copy(e, 0).start()
        plain_copy(e, 1).start()

    counter = [0]

    def remote(src, dst, device, sems):
        k = counter[0]
        counter[0] += 1
        return pltpu.make_async_remote_copy(
            src_ref=src, dst_ref=dst, send_sem=sems[0].at[k], recv_sem=sems[1].at[k],
            device_id=device, device_id_type=MESH,
        )

    def begin_far(i, carry):
        for e in range(1, xs):
            core_copy(e, i).start()
            own_copy(e, i).start()
        return carry

    def begin_near(i, carry):
        core_copy(0, i).start()
        own_copy(0, i).start()
        return carry

    def spread_piece(xx, zz):
        for e in range(1, ys):
            dens_y(e, xx, zz).start()
        dens_c(xx, zz, y).start()

    def launch_piece(xx):
        @pl.when(z < zs - 1)
        def _():
            dens_z(True, xx, z).start()

        @pl.when(z > 0)
        def _():
            dens_z(False, xx, z).start()

        spread_piece(xx, z)

    local.wait()
    launch_piece(x)
    lax.fori_loop(1, per, begin_far, 0)
    lax.fori_loop(0, per, begin_near, 0)

    pair_copy.wait()
    counts_copy.wait()

    base = 0
    for m in range(nblk):
        tall_here = (counts_ref[m] + 15) // 16
        lanes = counts_ref[pair_ref[0, m]]
        for j in range(1, neigh):
            lanes = lanes + counts_ref[pair_ref[j, m]]
        wide_here = (lanes + bs - 1) // bs
        if m % chip_blocks == 0:
            base = 0
        tiles_ref[m] = tall_here
        width_ref[m] = wide_here
        base_ref[m] = base
        base = base + tall_here * wide_here

    def take_tile(k, carry):
        mm = 0
        for q in range(1, chip_blocks):
            mm = mm + jnp.where(k >= base_ref[x * chip_blocks + q], 1, 0)
        at = k - base_ref[x * chip_blocks + mm]
        w = width_ref[x * chip_blocks + mm]
        down = 0
        for q in range(1, tall):
            down = down + jnp.where(at >= q * w, 1, 0)
        along = at - down * w
        take_ref[k] = jnp.where(along < w, (mm * neigh + along) * tall + down, 0)
        return carry

    lax.fori_loop(0, cap, take_tile, 0)

    def fill_pack(mm, carry):
        m = x * chip_blocks + mm
        slot = lax.broadcasted_iota(jnp.int32, (bs, 1), 0)
        place = lax.broadcasted_iota(jnp.int32, (bs, span), 1)
        at = 0
        for j in range(neigh):
            count = counts_ref[pair_ref[j, m]]
            goal = jnp.where(slot < count, slot + at, -1)
            pack[mm, j * bs:(j + 1) * bs, :] = jnp.where(goal == place, 1.0, 0.0).astype(pack.dtype)
            at = at + count
        return carry

    lax.fori_loop(0, chip_blocks, fill_pack, 0)

    def emit(i, carry):
        for e in range(1, xs):
            own_copy(e, i).wait()
            core_copy(e, i).wait_recv()

            def squeeze(mm, carry):
                left = jnp.concatenate([raw[e, i, mm, j] for j in range(neigh)], axis=1)
                close = jnp.dot(left, pack[mm], preferred_element_type=jnp.float32).astype(stage.dtype)
                for j in range(neigh):
                    stage[pl.ds((mm * neigh + j) * tall, tall)] = close[:, j * bs:(j + 1) * bs].reshape(tall, 16, bs)
                return carry

            lax.fori_loop(0, chip_blocks, squeeze, 0)

            def move(k, carry):
                for q in range(4):
                    outbox[e - 1, i, k * 4 + q] = stage[take_ref[k * 4 + q]]
                return carry

            lax.fori_loop(0, cap // 4, move, 0)
            x_copy(e, i).start()
        return carry

    for e in range(1, xs):
        dens_x(e).wait_recv()
        launch_piece(x_at(xs - e))
    lax.fori_loop(1, 2, emit, 0)

    def hop(h, carry):
        def pieces(k, carry):
            xx = x_at(k)

            @pl.when(z - h >= 0)
            def _():
                dens_z(True, xx, z - h).wait_recv()

                @pl.when(z < zs - 1)
                def _():
                    dens_z(True, xx, z - h).start()

                spread_piece(xx, z - h)

            @pl.when(z + h < zs)
            def _():
                dens_z(False, xx, z + h).wait_recv()

                @pl.when(z > 0)
                def _():
                    dens_z(False, xx, z + h).start()

                spread_piece(xx, z + h)

            return carry

        lax.fori_loop(0, xs, pieces, 0)
        from_y(h - 1)
        return carry

    def from_y(h):
        def pieces(k, carry):
            xx = x_at(k)

            def turn(zz):
                for e in range(1, ys):
                    dens_y(e, xx, zz).wait_recv()
                    dens_c(xx, zz, lax.rem(y + ys - e, ys)).start()

            @pl.when(z - h >= 0)
            def _():
                turn(z - h)

            @pl.when((z + h < zs) & (h > 0))
            def _():
                turn(z + h)

            return carry

        lax.fori_loop(0, xs, pieces, 0)

    total[...] = jnp.zeros_like(total)

    def fill_unpack(k, carry):
        m = lax.rem(x * chip_blocks + chip_blocks + k, nblk)
        slot = lax.broadcasted_iota(jnp.int32, (1, bs), 1)
        place = lax.broadcasted_iota(jnp.int32, (span, bs), 0)
        at = 0
        for j in range(neigh):
            count = counts_ref[pair_ref[j, m]]
            goal = jnp.where(slot < count, slot + at, -1)
            unpack[k, :, j * bs:(j + 1) * bs] = jnp.where(goal == place, 1.0, 0.0).astype(unpack.dtype)
            at = at + count
            for down in range(tall):
                inside = (j < width_ref[m]) & (down < tiles_ref[m])
                give_ref[(k * neigh + j) * tall + down] = jnp.where(
                    inside, base_ref[m] + down * width_ref[m] + j, 0
                )
        return carry

    lax.fori_loop(0, (xs - 1) * chip_blocks, fill_unpack, 0)

    for m in range(nblk):
        tens[m * slots + neigh] = jnp.zeros((bs, bs), tens.dtype)
        for n in range(nblk):
            found = neigh
            for j in range(neigh):
                found = jnp.where(pair_ref[j, m] == n, j, found)
            which_ref[m * nblk + n] = m * slots + found

    def hop_and_emit(h, carry):
        hop(h, carry)
        lax.fori_loop(jnp.minimum(h + 1, per), jnp.minimum(h + 2, per), emit, 0)
        return carry

    lax.fori_loop(1, zs, hop_and_emit, 0)
    from_y(zs - 1)
    lax.fori_loop(min(zs + 1, per), per, emit, 0)

    def settle(zz, carry):
        for xx in range(xs):
            for yy in range(ys):
                dens_c(xx, zz, yy).wait()
            for e in range(1, ys):
                dens_y(e, xx, zz).wait_send()

            @pl.when((z < zs - 1) & (zz <= z))
            def _():
                dens_z(True, xx, zz).wait_send()

            @pl.when((z > 0) & (zz >= z))
            def _():
                dens_z(False, xx, zz).wait_send()

        return carry

    lax.fori_loop(0, zs, settle, 0)
    for e in range(1, xs):
        dens_x(e).wait_send()

    lane = lax.broadcasted_iota(jnp.int32, (1, bs), 1)
    col_live = jnp.concatenate(
        [jnp.where(lane < counts_ref[b], 1.0, 0.0).astype(jnp.float32) for b in range(nblk)], axis=1
    )

    def mask_rows(b, carry):
        slot = lax.broadcasted_iota(jnp.int32, (bs, 1), 0)
        row_live = jnp.where(slot < counts_ref[b], 1.0, 0.0).astype(jnp.float32)
        dens[b] = (dens[b].astype(jnp.float32) * row_live * col_live).astype(dens.dtype)
        return carry

    lax.fori_loop(0, nblk, mask_rows, 0)

    side = nbf // 2
    cols = min(side, 512)

    def at_rows(first, count):
        return pl.ds(pl.multiple_of(first, 16), count)

    def take_near(i):
        own_copy(0, i).wait()
        core_copy(0, i).wait_recv()

        def put(mm, carry):
            for j in range(neigh):
                tens[(x * chip_blocks + mm) * slots + j] = raw[0, i, mm, j]
            return carry

        lax.fori_loop(0, chip_blocks, put, 0)

    def take_far(i):
        for r in range(xs - 1):
            x_copy(xs - 1 - r, i).wait_recv()
            arrived[...] = inbox[r, i]

            def spread(mm, carry):
                for q in range(neigh * tall):
                    stage[mm * neigh * tall + q] = arrived[give_ref[(r * chip_blocks + mm) * neigh * tall + q]]
                close = jnp.concatenate(
                    [stage[pl.ds((mm * neigh + j) * tall, tall)].reshape(bs, bs) for j in range(neigh)], axis=1
                )
                apart = jnp.dot(
                    close, unpack[r * chip_blocks + mm], preferred_element_type=jnp.float32
                ).astype(tens.dtype)
                for j in range(neigh):
                    tens[(x_at(r + 1) * chip_blocks + mm) * slots + j] = apart[:, j * bs:(j + 1) * bs]
                return carry

            lax.fori_loop(0, chip_blocks, spread, 0)

    def take_plain():
        for r in range(xs - 1):
            plain_arrival(r, 0).wait_recv()
            plain_arrival(r, 1).wait_recv()

            def put(mm, carry):
                for j in range(neigh):
                    tens[(x_at(r + 1) * chip_blocks + mm) * slots + j] = direct[r, mm, j]
                return carry

            lax.fori_loop(0, chip_blocks, put, 0)

    def first_half(first, count):
        def block_row(k, carry):
            m = lax.rem(first + k, nblk)
            left = jnp.concatenate([tens[m * slots + j] for j in range(neigh)], axis=1)
            near = jnp.concatenate([dens[pair_ref[j, m]] for j in range(neigh)], axis=0)
            h = jnp.dot(left, near, preferred_element_type=jnp.float32)
            at = pl.ds(pl.multiple_of(m * bs, bs), bs)
            half[at, :] = h.astype(half.dtype)
            for n in range(nblk):
                wide[at, n * bs:(n + 1) * bs] = tens[which_ref[m * nblk + n]]
            return carry

        lax.fori_loop(0, count, block_row, 0)

    def product(g, h):
        at = at_rows(g * group, group)
        for k in range(side // cols):
            lo = h * side + k * cols
            total[at, lo:lo + cols] += jnp.dot(
                half[at, :], wide[:, lo:lo + cols], preferred_element_type=jnp.float32
            )

    def one(i, carry):
        take_near(i)

        @pl.when(i == 0)
        def _():
            take_plain()

        @pl.when(i > 0)
        def _():
            take_far(i)

        first_half(0, nblk)

        def second_half(g, carry):
            product(g, 0)
            product(g, 1)
            return carry

        lax.fori_loop(0, atoms, second_half, 0)
        return carry

    lax.fori_loop(0, per - 1, one, 0)

    counter[0] = 0
    ksems = (k_send, k_recv)
    sends = []

    def send_to(src, dst, device):
        cp = remote(src, dst, device, ksems)
        cp.start()
        sends.append(cp)
        return cp

    def part_product(g, q, h):
        at = at_rows(g * group, group)
        qt = at_rows(q * chip_blocks * bs, chip_blocks * bs)
        qc = pl.ds(pl.multiple_of(q * chip_blocks * bs, 128), chip_blocks * bs)
        for k in range(side // cols):
            lo = h * side + k * cols
            total[at, lo:lo + cols] += jnp.dot(
                half[at, qc], wide[qt, lo:lo + cols], preferred_element_type=jnp.float32
            )

    take_near(per - 1)
    first_half(x * chip_blocks, chip_blocks)
    for core in (0, 1):
        for h in (0, 1):
            part_product(x * 2 + core, x, h)
    take_far(per - 1)
    first_half((x + 1) * chip_blocks, nblk - chip_blocks)

    def last_product(e, core, h):
        if e:
            product(x_at(e) * 2 + core, h)
        else:
            for f in range(1, xs):
                part_product(x * 2 + core, x_at(f), h)

    left, right = slice(0, side), slice(side, nbf)

    def y_at(e):
        return lax.rem(y + e, ys)

    core_left, core_right = {}, {}
    for e in list(range(1, xs)) + [0]:
        last_product(e, other, 0)
        last_product(e, other, 1)
        for store, part in ((core_left, left), (core_right, right)):
            store[e] = send_to(
                total.at[at_rows((x_at(e) * 2 + other) * group, group), part],
                from_core.at[e * group:(e + 1) * group, part],
                sibling,
            )

    def core_sum(e, row, count, part):
        return (
            total[at_rows((x_at(e) * 2 + c) * group + row, count), part]
            + from_core[at_rows(e * group + row, count), part]
        )

    zr = zs * rows
    left_x = {}
    for e in range(1, xs):
        last_product(e, c, 0)
        core_left[e].wait_recv()
        for f in list(range(1, ys)) + [0]:
            lo = (e - 1) * group + f * zr
            for zz in range(zs):
                send[lo + zz * rows:lo + (zz + 1) * rows, left] = core_sum(
                    e, (zz * ys + y_at(f)) * rows, rows, left
                ).astype(send.dtype)
            left_x[e, f] = send_to(
                send.at[lo:lo + zr, left], first_x.at[lo:lo + zr, :], (x_at(e) * 2 + c, u)
            )
    right_y = {}
    for e in list(range(1, xs)) + [0]:
        last_product(e, c, 1)
        core_right[e].wait_recv()
        for f in range(1, ys):
            lo = ((f - 1) * xs + e) * zr
            to = (f - 1) * xs * zr + x_at(e) * zr
            for zz in range(zs):
                send[lo + zz * rows:lo + (zz + 1) * rows, right] = core_sum(
                    e, (zz * ys + y_at(f)) * rows, rows, right
                ).astype(send.dtype)
            right_y[f, e] = send_to(
                send.at[lo:lo + zr, right], second_y.at[at_rows(to, zr), :], (t, y_peer(f))
            )
    last_product(0, c, 0)
    core_left[0].wait_recv()

    def left_after_x(zz, f):
        value = core_sum(0, (zz * ys + y_at(f)) * rows, rows, left)
        for e in range(xs - 1):
            row = e * group + f * zr + zz * rows
            value = value + first_x[at_rows(row, rows), :].astype(jnp.float32)
        return value

    stage = max((xs - 1) * group, (ys - 1) * xs * zr)
    left_y = []
    for f in range(1, ys):
        lo = stage + (f - 1) * zr
        for e in range(1, xs):
            left_x[e, f].wait_recv()
        for zz in range(zs):
            send[lo + zz * rows:lo + (zz + 1) * rows, left] = left_after_x(zz, f).astype(send.dtype)
        left_y.append(send_to(
            send.at[lo:lo + zr, left], first_y.at[(f - 1) * zr:f * zr, :], (t, y_peer(f))
        ))

    def right_after_y(e, zz):
        value = core_sum(e, (zz * ys + y) * rows, rows, right)
        for f in range(ys - 1):
            row = f * xs * zr + x_at(e) * zr + zz * rows
            value = value + second_y[at_rows(row, rows), :].astype(jnp.float32)
        return value

    right_x = []
    for e in range(1, xs):
        lo = stage + (e - 1) * zr
        for f in range(1, ys):
            right_y[f, e].wait_recv()
        for zz in range(zs):
            send[lo + zz * rows:lo + (zz + 1) * rows, right] = right_after_y(e, zz).astype(send.dtype)
        right_x.append(send_to(
            send.at[lo:lo + zr, right], second_x.at[(e - 1) * zr:e * zr, :], (x_at(e) * 2 + c, u)
        ))

    def left_after_y(zz):
        value = left_after_x(zz, 0)
        for f in range(ys - 1):
            value = value + first_y[at_rows(f * zr + zz * rows, rows), :].astype(jnp.float32)
        return value

    def right_after_x(zz):
        value = right_after_y(0, zz)
        for e in range(xs - 1):
            value = value + second_x[at_rows(e * zr + zz * rows, rows), :].astype(jnp.float32)
        return value

    stage = stage + max(xs - 1, ys - 1) * zr
    ends = []
    for waits, after, into, part in (
        (left_y, left_after_y, first_z, left), (right_x, right_after_x, second_z, right)
    ):
        for cp in waits:
            cp.wait_recv()
        if part == right:
            for f in range(1, ys):
                right_y[f, 0].wait_recv()
        else:
            for e in range(1, xs):
                left_x[e, 0].wait_recv()
        arrivals = []
        for e in range(1, zs):
            lo = stage + (e - 1) * rows
            send[lo:lo + rows, part] = after(lax.rem(z + e, zs)).astype(send.dtype)
            arrivals.append(send_to(
                send.at[lo:lo + rows, part], into.at[(e - 1) * rows:e * rows, :], (t, z_peer(e))
            ))
        ends.append((arrivals, after, into, part))
    block = mine // bs
    slot = lax.broadcasted_iota(jnp.int32, (rows, 1), 0) + mine % bs
    row_live = jnp.where(slot < counts_ref[block], 1.0, 0.0).astype(jnp.float32)
    for arrivals, after, into, part in ends:
        value = after(z)
        for e in range(zs - 1):
            arrivals[e].wait_recv()
            value = value + into[e * rows:(e + 1) * rows, :].astype(jnp.float32)
        out_ref[:, part] = value * row_live * col_live[:, part]
    for cp in sends:
        cp.wait_send()

    def finish(i, carry):
        core_copy(0, i).wait_send()

        @pl.when(i > 0)
        def _():
            for e in range(1, xs):
                core_copy(e, i).wait_send()
                x_copy(e, i).wait_send()

        return carry

    lax.fori_loop(0, per, finish, 0)
    for e in range(1, xs):
        plain_copy(e, 0).wait_send()
        plain_copy(e, 1).wait_send()


def packed_caps(chip_blocks, neigh, bs):
    full = chip_blocks * neigh * (bs // 16)
    return [full * k // 32 // 4 * 4 for k in (22, 24, 26, 28)] + [full]


def packed_scratch(cap, atoms, aux, xs, ys, zs, per, nblk, neigh, bs, rows):
    nbf, chip_blocks, group = nblk * bs, nblk // xs, aux * rows
    side, zr, span, tall = nbf // 2, zs * rows, neigh * bs, bs // 16
    n_k = 2 * (xs + (xs - 1) + (ys - 1) + (zs - 1)) + 2 * (xs - 1) * (ys - 1)
    send_rows = max((xs - 1) * group, (ys - 1) * xs * zr) + max(xs - 1, ys - 1) * zr + zr
    vmem, smem, dma = pltpu.VMEM, pltpu.SMEM, pltpu.SemaphoreType.DMA
    bf16, f32 = jnp.bfloat16, jnp.float32
    far = max(xs - 1, 1)
    return [
        smem((neigh, nblk), jnp.int32),
        smem((nblk,), jnp.int32),
        smem((nblk,), jnp.int32),
        smem((nblk,), jnp.int32),
        smem((nblk,), jnp.int32),
        smem((cap,), jnp.int32),
        smem((far * chip_blocks * neigh * tall,), jnp.int32),
        smem((nblk * nblk,), jnp.int32),
        vmem((nblk, bs, nbf), bf16),
        vmem((xs, per, chip_blocks, neigh, bs, bs), bf16),
        vmem((far, chip_blocks, neigh, bs, bs), bf16),
        vmem((far, per, cap, 16, bs), bf16),
        vmem((far, per, cap, 16, bs), bf16),
        vmem((chip_blocks * neigh * tall, 16, bs), bf16),
        vmem((cap, 16, bs), bf16),
        vmem((nblk * (neigh + 1), bs, bs), bf16),
        vmem((chip_blocks, span, span), bf16),
        vmem((far * chip_blocks, span, span), bf16),
        vmem((nbf, nbf), bf16),
        vmem((nbf, nbf), bf16),
        vmem((send_rows, nbf), bf16),
        vmem((nbf, nbf), f32),
        vmem((xs * group, nbf), f32),
        vmem((far * group, side), bf16),
        vmem((max(ys - 1, 1) * zr, side), bf16),
        vmem((max(zs - 1, 1) * rows, side), bf16),
        vmem((max(ys - 1, 1) * xs * zr, side), bf16),
        vmem((far * zr, side), bf16),
        vmem((max(zs - 1, 1) * rows, side), bf16),
        dma((xs, per)),
        dma,
        dma,
        dma,
        dma((xs, per)),
        dma((xs, per)),
        dma((far, 2)),
        dma((far, 2)),
        dma((far, per)),
        dma((far, per)),
        dma((far,)),
        dma((far,)),
        dma((2, zs, xs)),
        dma((zs, xs)),
        dma((zs, xs, max(ys - 1, 1))),
        dma((zs, xs, max(ys - 1, 1))),
        dma((zs, ys, xs)),
        dma((zs, ys, xs)),
        dma((n_k,)),
        dma((n_k,)),
    ]


VMEM_BYTES = 67043328


def packed_call(which, cap, sizes, three_index, density, pair_blocks, basis_counts):
    atoms, aux, xs, ys, zs = sizes[:5]
    rows, nbf = density.shape
    anywhere = pl.BlockSpec(memory_space=pl.ANY)
    return pl.pallas_call(
        functools.partial(packed_kernel, cap, atoms, aux, xs, ys, zs),
        out_shape=jax.ShapeDtypeStruct((rows, nbf), jnp.float32),
        in_specs=[anywhere] * 4,
        out_specs=pl.BlockSpec(memory_space=pltpu.VMEM),
        scratch_shapes=packed_scratch(cap, *sizes),
        compiler_params=pltpu.CompilerParams(
            collective_id=which, has_side_effects=True, vmem_limit_bytes=VMEM_BYTES
        ),
    )(pair_blocks.T, basis_counts, three_index, density)


def per_device(atoms, aux, three_index, density, pair_blocks, basis_counts):
    aux_here, own_blocks, neigh, bs, _ = three_index.shape
    rows, nbf = density.shape
    nblk = nbf // bs
    xs = atoms // 2
    ys = xs if aux % xs == 0 else 1
    zs = aux // ys
    per = aux_here // atoms
    sizes = (atoms, aux, xs, ys, zs, per, nblk, neigh, bs, rows)
    caps = packed_caps(nblk // xs, neigh, bs)
    need = sum(
        math.prod(ref.shape) * jnp.dtype(ref.dtype).itemsize
        for ref in packed_scratch(caps[-1], *sizes) if getattr(ref, 'memory_space', None) == pltpu.VMEM
    )
    if per < 2 or need + 2 * rows * nbf * 4 > VMEM_BYTES - 2**21:
        return plain_device(atoms, aux, three_index, density, pair_blocks, basis_counts)
    hit = pair_blocks[:, :, None] == jnp.arange(nblk)[None, None, :]
    lanes = jnp.sum(jnp.where(hit, basis_counts[None, None, :], 0), axis=(1, 2))
    tiles = ((basis_counts + 15) >> 4) * ((lanes + bs - 1) // bs)
    chip = jnp.max(jnp.sum(tiles.reshape(xs, nblk // xs), axis=1))
    choice = sum((chip > cap).astype(jnp.int32) for cap in caps[:-1])
    branches = [functools.partial(packed_call, k, cap, sizes) for k, cap in enumerate(caps)]
    return lax.switch(choice, branches, three_index, density, pair_blocks, basis_counts)


def solution(mesh):
    in_specs = (P("aux", "atom", None, None, None), P(("atom", "aux"), None), P(), P())
    out_specs = P(("atom", "aux"), None)
    return jax.shard_map(
        functools.partial(per_device, mesh.shape["atom"], mesh.shape["aux"]),
        mesh=mesh, in_specs=in_specs, out_specs=out_specs, check_vma=False,
    )
```

```python
import functools
import math

import jax
import jax.numpy as jnp
from jax import lax
from jax.experimental import pallas as pl
from jax.experimental.pallas import tpu as pltpu
from jax.sharding import PartitionSpec as P

MESH = pl.DeviceIdType.MESH


def kernel(
    atoms, aux, xs, ys, zs,
    pair_hbm, counts_hbm, tensor_ref, piece_ref, out_ref,
    pair_ref, counts_ref, dens, tens, wide, half, send, total, from_core,
    first_x, first_y, first_z, second_y, second_x, second_z,
    own_sem, piece_sem, pair_sem, counts_sem, t_send, t_recv, d_send, d_recv, k_send, k_recv,
):
    per, nblk, neigh, bs = tens.shape[0], tens.shape[1], tens.shape[2], tens.shape[3]
    nbf = total.shape[1]
    own_blocks = nblk // atoms
    rows = piece_ref.shape[0]
    group = aux * rows
    t = lax.axis_index("atom")
    u = lax.axis_index("aux")
    x, c = t // 2, t % 2
    z, y = u // ys, u % ys

    pair_copy = pltpu.make_async_copy(pair_hbm, pair_ref, pair_sem)
    counts_copy = pltpu.make_async_copy(counts_hbm, counts_ref, counts_sem)
    pair_copy.start()
    counts_copy.start()

    def atom_peer(d):
        return lax.rem(t + d, atoms)

    def x_peer(e):
        return lax.rem(x + e, xs) * 2 + c

    def y_peer(e):
        return z * ys + lax.rem(y + e, ys)

    def z_peer(e):
        return lax.rem(z + e, zs) * ys + y

    barrier = pltpu.get_barrier_semaphore()
    for d in range(1, atoms):
        pl.semaphore_signal(barrier, inc=1, device_id=(atom_peer(d), u), device_id_type=MESH)
    for e in range(1, ys):
        pl.semaphore_signal(barrier, inc=1, device_id=(t, y_peer(e)), device_id_type=MESH)
    for e in range(1, zs):
        pl.semaphore_signal(barrier, inc=1, device_id=(t, z_peer(e)), device_id_type=MESH)
    pl.semaphore_wait(barrier, (atoms - 1) + (ys - 1) + (zs - 1))

    counter = [0]

    def remote(src, dst, device, sems):
        k = counter[0]
        counter[0] += 1
        return pltpu.make_async_remote_copy(
            src_ref=src, dst_ref=dst, send_sem=sems[0].at[k], recv_sem=sems[1].at[k],
            device_id=device, device_id_type=MESH,
        )

    dsems = (d_send, d_recv)

    def dens_rows(first, count):
        return dens.at[first // bs, pl.ds(pl.multiple_of(first % bs, 16), count), :]

    mine = (t * aux + u) * rows
    local = pltpu.make_async_copy(piece_ref, dens_rows(mine, rows), piece_sem)
    local.start()
    over_x = []
    for e in range(1, xs):
        cp = remote(piece_ref, dens_rows(mine, rows), (x_peer(e), u), dsems)
        cp.start()
        over_x.append(cp)

    def own_copy(i):
        return pltpu.make_async_copy(
            tensor_ref.at[t * per + i], tens.at[i, pl.ds(t * own_blocks, own_blocks)], own_sem.at[i]
        )

    def t_copy(i, d):
        to = atom_peer(d)
        return pltpu.make_async_remote_copy(
            src_ref=tensor_ref.at[to * per + i],
            dst_ref=tens.at[i, pl.ds(t * own_blocks, own_blocks)],
            send_sem=t_send.at[i, d - 1],
            recv_sem=t_recv.at[i, d - 1],
            device_id=(to, u),
            device_id_type=MESH,
        )

    order = list(range(1, atoms, 2)) + list(range(2, atoms, 2))

    def begin(i, carry):
        for d in order:
            t_copy(i, d).start()
        own_copy(i).start()
        return carry

    lax.fori_loop(0, per, begin, 0)

    local.wait()
    for cp in over_x:
        cp.wait()
    over_y = []
    for xx in range(xs):
        first = ((xx * 2 + c) * aux + u) * rows
        for e in range(1, ys):
            cp = remote(dens_rows(first, rows), dens_rows(first, rows), (t, y_peer(e)), dsems)
            cp.start()
            over_y.append(cp)
    total[...] = jnp.zeros_like(total)
    for cp in over_y:
        cp.wait()
    over_z = []
    for xx in range(xs):
        first = ((xx * 2 + c) * aux + z * ys) * rows
        for e in range(1, zs):
            cp = remote(dens_rows(first, ys * rows), dens_rows(first, ys * rows), (t, z_peer(e)), dsems)
            cp.start()
            over_z.append(cp)
    for cp in over_z:
        cp.wait()
    over_c = []
    for xx in range(xs):
        blocks = dens.at[pl.ds((xx * 2 + c) * own_blocks, own_blocks)]
        cp = remote(blocks, blocks, (x * 2 + (1 - c), u), dsems)
        cp.start()
        over_c.append(cp)
    for cp in over_c:
        cp.wait()

    pair_copy.wait()
    counts_copy.wait()
    lane = lax.broadcasted_iota(jnp.int32, (1, bs), 1)
    col_live = jnp.concatenate(
        [jnp.where(lane < counts_ref[b], 1.0, 0.0).astype(jnp.float32) for b in range(nblk)], axis=1
    )

    def mask_rows(b, carry):
        slot = lax.broadcasted_iota(jnp.int32, (bs, 1), 0)
        row_live = jnp.where(slot < counts_ref[b], 1.0, 0.0).astype(jnp.float32)
        dens[b] = (dens[b].astype(jnp.float32) * row_live * col_live).astype(dens.dtype)
        return carry

    lax.fori_loop(0, nblk, mask_rows, 0)

    side = nbf // 2
    cols = min(side, 512)

    def at_rows(first, count):
        return pl.ds(pl.multiple_of(first, 16), count)

    def arrive(i):
        own_copy(i).wait()
        for d in range(1, atoms):
            t_copy(i, d).wait_recv()

    def first_half(i, first, count):
        def block_row(k, carry):
            m = first + k
            left = jnp.concatenate([tens[i, m, j] for j in range(neigh)], axis=1)
            right = jnp.concatenate([dens[pair_ref[j, m]] for j in range(neigh)], axis=0)
            h = jnp.dot(left, right, preferred_element_type=jnp.float32)
            at = pl.ds(pl.multiple_of(m * bs, bs), bs)
            half[at, :] = h.astype(half.dtype)
            for n in range(nblk):
                block = jnp.zeros((bs, bs), wide.dtype)
                for j in range(neigh):
                    block = jnp.where(pair_ref[j, m] == n, tens[i, m, j], block)
                wide[at, n * bs:(n + 1) * bs] = block
            return carry

        lax.fori_loop(0, count, block_row, 0)

    def product(g, h):
        at = at_rows(g * group, group)
        for k in range(side // cols):
            lo = h * side + k * cols
            total[at, lo:lo + cols] += jnp.dot(
                half[at, :], wide[:, lo:lo + cols], preferred_element_type=jnp.float32
            )

    def one(i, carry):
        arrive(i)
        first_half(i, 0, nblk)

        def second_half(g, carry):
            product(g, 0)
            product(g, 1)
            return carry

        lax.fori_loop(0, atoms, second_half, 0)
        return carry

    lax.fori_loop(0, per - 1, one, 0)

    counter[0] = 0
    ksems = (k_send, k_recv)
    sends = []

    def send_to(src, dst, device):
        cp = remote(src, dst, device, ksems)
        cp.start()
        sends.append(cp)
        return cp

    other = 1 - c
    sibling = (x * 2 + other, u)
    final = per - 1
    own_copy(final).wait()
    for d in order[:-1]:
        t_copy(final, d).wait_recv()
    late = lax.rem(t + atoms - order[-1], atoms)

    def part_product(g, q, h):
        at, qt = at_rows(g * group, group), at_rows(q * group, group)
        qc = pl.ds(pl.multiple_of(q * group, 128), group)
        for k in range(side // cols):
            lo = h * side + k * cols
            total[at, lo:lo + cols] += jnp.dot(
                half[at, qc], wide[qt, lo:lo + cols], preferred_element_type=jnp.float32
            )

    def early_rows(k, carry):
        first_half(final, lax.rem(late + k, atoms) * own_blocks, own_blocks)
        return carry

    lax.fori_loop(1, atoms, early_rows, 0)

    def early_products(k, carry):
        g = (k // (atoms - 1)) * 2 + other
        q = lax.rem(late + 1 + k % (atoms - 1), atoms)
        part_product(g, q, 0)
        part_product(g, q, 1)
        return carry

    lax.fori_loop(0, xs * (atoms - 1), early_products, 0)
    t_copy(final, order[-1]).wait_recv()
    first_half(final, late * own_blocks, own_blocks)

    def last_product(e, core, h):
        if core is c:
            product(x_at(e) * 2 + c, h)
        else:
            part_product(x_at(e) * 2 + other, late, h)

    left, right = slice(0, side), slice(side, nbf)

    def x_at(e):
        return lax.rem(x + e, xs)

    def y_at(e):
        return lax.rem(y + e, ys)

    core_left, core_right = {}, {}
    for e in list(range(1, xs)) + [0]:
        last_product(e, other, 0)
        last_product(e, other, 1)
        for store, part in ((core_left, left), (core_right, right)):
            store[e] = send_to(
                total.at[at_rows((x_at(e) * 2 + other) * group, group), part],
                from_core.at[e * group:(e + 1) * group, part],
                sibling,
            )

    def core_sum(e, row, count, part):
        return (
            total[at_rows((x_at(e) * 2 + c) * group + row, count), part]
            + from_core[at_rows(e * group + row, count), part]
        )

    zr = zs * rows
    left_x = {}
    for e in range(1, xs):
        last_product(e, c, 0)
        core_left[e].wait_recv()
        for f in list(range(1, ys)) + [0]:
            lo = (e - 1) * group + f * zr
            for zz in range(zs):
                send[lo + zz * rows:lo + (zz + 1) * rows, left] = core_sum(
                    e, (zz * ys + y_at(f)) * rows, rows, left
                ).astype(send.dtype)
            left_x[e, f] = send_to(
                send.at[lo:lo + zr, left], first_x.at[lo:lo + zr, :], (x_at(e) * 2 + c, u)
            )
    right_y = {}
    for e in list(range(1, xs)) + [0]:
        last_product(e, c, 1)
        core_right[e].wait_recv()
        for f in range(1, ys):
            lo = ((f - 1) * xs + e) * zr
            to = (f - 1) * xs * zr + x_at(e) * zr
            for zz in range(zs):
                send[lo + zz * rows:lo + (zz + 1) * rows, right] = core_sum(
                    e, (zz * ys + y_at(f)) * rows, rows, right
                ).astype(send.dtype)
            right_y[f, e] = send_to(
                send.at[lo:lo + zr, right], second_y.at[at_rows(to, zr), :], (t, y_peer(f))
            )
    last_product(0, c, 0)
    core_left[0].wait_recv()

    def left_after_x(zz, f):
        value = core_sum(0, (zz * ys + y_at(f)) * rows, rows, left)
        for e in range(xs - 1):
            row = e * group + f * zr + zz * rows
            value = value + first_x[at_rows(row, rows), :].astype(jnp.float32)
        return value

    stage = max((xs - 1) * group, (ys - 1) * xs * zr)
    left_y = []
    for f in range(1, ys):
        lo = stage + (f - 1) * zr
        for e in range(1, xs):
            left_x[e, f].wait_recv()
        for zz in range(zs):
            send[lo + zz * rows:lo + (zz + 1) * rows, left] = left_after_x(zz, f).astype(send.dtype)
        left_y.append(send_to(
            send.at[lo:lo + zr, left], first_y.at[(f - 1) * zr:f * zr, :], (t, y_peer(f))
        ))

    def right_after_y(e, zz):
        value = core_sum(e, (zz * ys + y) * rows, rows, right)
        for f in range(ys - 1):
            row = f * xs * zr + x_at(e) * zr + zz * rows
            value = value + second_y[at_rows(row, rows), :].astype(jnp.float32)
        return value

    right_x = []
    for e in range(1, xs):
        lo = stage + (e - 1) * zr
        for f in range(1, ys):
            right_y[f, e].wait_recv()
        for zz in range(zs):
            send[lo + zz * rows:lo + (zz + 1) * rows, right] = right_after_y(e, zz).astype(send.dtype)
        right_x.append(send_to(
            send.at[lo:lo + zr, right], second_x.at[(e - 1) * zr:e * zr, :], (x_at(e) * 2 + c, u)
        ))

    def left_after_y(zz):
        value = left_after_x(zz, 0)
        for f in range(ys - 1):
            value = value + first_y[at_rows(f * zr + zz * rows, rows), :].astype(jnp.float32)
        return value

    def right_after_x(zz):
        value = right_after_y(0, zz)
        for e in range(xs - 1):
            value = value + second_x[at_rows(e * zr + zz * rows, rows), :].astype(jnp.float32)
        return value

    stage = stage + max(xs - 1, ys - 1) * zr
    ends = []
    for waits, after, into, part in (
        (left_y, left_after_y, first_z, left), (right_x, right_after_x, second_z, right)
    ):
        for cp in waits:
            cp.wait_recv()
        if part == right:
            for f in range(1, ys):
                right_y[f, 0].wait_recv()
        else:
            for e in range(1, xs):
                left_x[e, 0].wait_recv()
        arrivals = []
        for e in range(1, zs):
            lo = stage + (e - 1) * rows
            send[lo:lo + rows, part] = after(lax.rem(z + e, zs)).astype(send.dtype)
            arrivals.append(send_to(
                send.at[lo:lo + rows, part], into.at[(e - 1) * rows:e * rows, :], (t, z_peer(e))
            ))
        ends.append((arrivals, after, into, part))
    block = mine // bs
    slot = lax.broadcasted_iota(jnp.int32, (rows, 1), 0) + mine % bs
    row_live = jnp.where(slot < counts_ref[block], 1.0, 0.0).astype(jnp.float32)
    for arrivals, after, into, part in ends:
        value = after(z)
        for e in range(zs - 1):
            arrivals[e].wait_recv()
            value = value + into[e * rows:(e + 1) * rows, :].astype(jnp.float32)
        out_ref[:, part] = value * row_live * col_live[:, part]
    for cp in sends:
        cp.wait_send()

    def finish(i, carry):
        for d in range(1, atoms):
            t_copy(i, d).wait_send()
        return carry

    lax.fori_loop(0, per, finish, 0)


def plain_device(atoms, aux, three_index, density, pair_blocks, basis_counts):
    aux_here, own_blocks, neigh, bs, _ = three_index.shape
    rows, nbf = density.shape
    nblk = nbf // bs
    xs = atoms // 2
    ys = xs if aux % xs == 0 else 1
    zs = aux // ys
    per = aux_here // atoms
    group = aux * rows
    n_d = (xs - 1) + xs * (ys - 1) + xs * (zs - 1) + xs
    n_k = 2 * (xs + (xs - 1) + (ys - 1) + (zs - 1)) + 2 * (xs - 1) * (ys - 1)
    side = nbf // 2
    zr = zs * rows
    send_rows = max((xs - 1) * group, (ys - 1) * xs * zr) + max(xs - 1, ys - 1) * zr + zr
    vmem, dma = pltpu.VMEM, pltpu.SemaphoreType.DMA
    bf16, f32 = jnp.bfloat16, jnp.float32
    return pl.pallas_call(
        functools.partial(kernel, atoms, aux, xs, ys, zs),
        out_shape=jax.ShapeDtypeStruct((rows, nbf), f32),
        in_specs=[
            pl.BlockSpec(memory_space=pl.ANY),
            pl.BlockSpec(memory_space=pl.ANY),
            pl.BlockSpec(memory_space=pl.ANY),
            pl.BlockSpec(memory_space=pl.ANY),
        ],
        out_specs=pl.BlockSpec(memory_space=pltpu.VMEM),
        scratch_shapes=[
            pltpu.SMEM(pair_blocks.shape[::-1], jnp.int32),
            pltpu.SMEM(basis_counts.shape, jnp.int32),
            vmem((nblk, bs, nbf), bf16),
            vmem((per, nblk, neigh, bs, bs), bf16),
            vmem((nbf, nbf), bf16),
            vmem((nbf, nbf), bf16),
            vmem((send_rows, nbf), bf16),
            vmem((nbf, nbf), f32),
            vmem((xs * group, nbf), f32),
            vmem((max(xs - 1, 1) * group, side), bf16),
            vmem((max(ys - 1, 1) * zs * rows, side), bf16),
            vmem((max(zs - 1, 1) * rows, side), bf16),
            vmem((max(ys - 1, 1) * xs * zs * rows, side), bf16),
            vmem((max(xs - 1, 1) * zs * rows, side), bf16),
            vmem((max(zs - 1, 1) * rows, side), bf16),
            dma((per,)),
            dma,
            dma,
            dma,
            dma((per, atoms - 1)),
            dma((per, atoms - 1)),
            dma((n_d,)),
            dma((n_d,)),
            dma((n_k,)),
            dma((n_k,)),
        ],
        compiler_params=pltpu.CompilerParams(
            collective_id=0, has_side_effects=True, vmem_limit_bytes=67043328
        ),
    )(pair_blocks.T, basis_counts, three_index, density)


def packed_kernel(
    cap, atoms, aux, xs, ys, zs,
    pair_hbm, counts_hbm, tensor_ref, piece_ref, out_ref,
    pair_ref, counts_ref, tiles_ref, width_ref, base_ref, start_ref, take_ref, give_ref,
    dens, raw, direct, outbox, inbox, stage, arrived, pack, place, lift, near,
    wide, half, send, total, from_core,
    first_x, first_y, first_z, second_y, second_x, second_z, cut,
    own_sem, piece_sem, pair_sem, counts_sem, t_send, t_recv, p_send, p_recv, x_send, x_recv, dx_send, dx_recv, dz_send, dz_recv, dy_send, dy_recv,
    dc_send, dc_recv, k_send, k_recv,
):
    per, chip_blocks, neigh, bs = raw.shape[1], raw.shape[2], raw.shape[3], raw.shape[4]
    nbf, live = half.shape[1], total.shape[1]
    nblk = nbf // bs
    own_blocks = nblk // atoms
    rows = piece_ref.shape[0]
    group = aux * rows
    tall = bs // 16
    span = neigh * bs
    t = lax.axis_index("atom")
    u = lax.axis_index("aux")
    x, c = t // 2, t % 2
    z, y = u // ys, u % ys
    other = 1 - c
    sibling = (x * 2 + other, u)

    pair_copy = pltpu.make_async_copy(pair_hbm, pair_ref, pair_sem)
    counts_copy = pltpu.make_async_copy(counts_hbm, counts_ref, counts_sem)
    pair_copy.start()
    counts_copy.start()

    def x_at(e):
        return lax.rem(x + e, xs)

    def x_peer(e):
        return x_at(e) * 2 + c

    def y_peer(e):
        return z * ys + lax.rem(y + e, ys)

    def z_peer(e):
        return lax.rem(z + e, zs) * ys + y

    def own_copy(e, i):
        return pltpu.make_async_copy(
            tensor_ref.at[x_peer(e) * per + i], raw.at[e, i, pl.ds(c * own_blocks, own_blocks)], own_sem.at[e, i]
        )

    def core_copy(e, i):
        return pltpu.make_async_remote_copy(
            src_ref=tensor_ref.at[(x_at(e) * 2 + other) * per + i],
            dst_ref=raw.at[e, i, pl.ds(c * own_blocks, own_blocks)],
            send_sem=t_send.at[e, i], recv_sem=t_recv.at[e, i],
            device_id=sibling, device_id_type=MESH,
        )

    def x_copy(e, i):
        return pltpu.make_async_remote_copy(
            src_ref=outbox.at[e - 1, i], dst_ref=inbox.at[xs - e - 1, i],
            send_sem=x_send.at[e - 1, i], recv_sem=x_recv.at[xs - e - 1, i],
            device_id=(x_peer(e), u), device_id_type=MESH,
        )

    def plain_copy(e, core):
        return pltpu.make_async_remote_copy(
            src_ref=tensor_ref.at[(x_at(e) * 2 + core) * per],
            dst_ref=direct.at[xs - e - 1, pl.ds(c * own_blocks, own_blocks)],
            send_sem=p_send.at[e - 1, core], recv_sem=p_recv.at[xs - e - 1, c],
            device_id=(x_at(e) * 2 + core, u), device_id_type=MESH,
        )

    def plain_arrival(r, core):
        here = direct.at[r, pl.ds(core * own_blocks, own_blocks)]
        return pltpu.make_async_remote_copy(
            src_ref=here, dst_ref=here, send_sem=p_send.at[r, core], recv_sem=p_recv.at[r, core],
            device_id=sibling, device_id_type=MESH,
        )

    def piece(xx, zz, yy):
        first = ((xx * 2 + c) * aux + zz * ys + yy) * rows
        return dens.at[pl.ds(pl.multiple_of(first, 16), rows), :]

    def dens_copy(xx, zz, yy, device, send_sem, recv_sem):
        return pltpu.make_async_remote_copy(
            src_ref=piece(xx, zz, yy), dst_ref=piece(xx, zz, yy), send_sem=send_sem, recv_sem=recv_sem,
            device_id=device, device_id_type=MESH,
        )

    def dens_x(e):
        return pltpu.make_async_remote_copy(
            src_ref=piece_ref, dst_ref=piece(x, z, y), send_sem=dx_send.at[e - 1], recv_sem=dx_recv.at[e - 1],
            device_id=(x_peer(e), u), device_id_type=MESH,
        )

    def dens_z(up, xx, zz):
        to = (z + 1 if up else z - 1) * ys + y
        return dens_copy(xx, zz, y, (t, to), dz_send.at[int(up), zz, xx], dz_recv.at[zz, xx])

    def dens_y(e, xx, zz):
        return dens_copy(xx, zz, y, (t, y_peer(e)), dy_send.at[zz, xx, e - 1], dy_recv.at[zz, xx, e - 1])

    def dens_c(xx, zz, yy):
        return dens_copy(xx, zz, yy, sibling, dc_send.at[zz, yy, xx], dc_recv.at[zz, yy, xx])

    mine = (t * aux + u) * rows
    barrier = pltpu.get_barrier_semaphore()
    pl.semaphore_signal(barrier, inc=1, device_id=sibling, device_id_type=MESH)
    for e in range(1, xs):
        pl.semaphore_signal(barrier, inc=1, device_id=(x_peer(e), u), device_id_type=MESH)
        pl.semaphore_signal(barrier, inc=1, device_id=(x_at(e) * 2 + other, u), device_id_type=MESH)
    for e in range(1, ys):
        pl.semaphore_signal(barrier, inc=1, device_id=(t, y_peer(e)), device_id_type=MESH)
    for e in range(1, zs):
        pl.semaphore_signal(barrier, inc=1, device_id=(t, z_peer(e)), device_id_type=MESH)
    local = pltpu.make_async_copy(piece_ref, piece(x, z, y), piece_sem)
    local.start()
    pl.semaphore_wait(barrier, 1 + 2 * (xs - 1) + (ys - 1) + (zs - 1))

    for e in range(1, xs):
        dens_x(e).start()
    for e in range(1, xs):
        plain_copy(e, 0).start()
        plain_copy(e, 1).start()

    counter = [0]

    def remote(src, dst, device, sems):
        k = counter[0]
        counter[0] += 1
        return pltpu.make_async_remote_copy(
            src_ref=src, dst_ref=dst, send_sem=sems[0].at[k], recv_sem=sems[1].at[k],
            device_id=device, device_id_type=MESH,
        )

    def begin_far(i, carry):
        for e in range(1, xs):
            core_copy(e, i).start()
            own_copy(e, i).start()
        return carry

    def begin_near(i, carry):
        core_copy(0, i).start()
        own_copy(0, i).start()
        return carry

    def spread_piece(xx, zz):
        for e in range(1, ys):
            dens_y(e, xx, zz).start()
        dens_c(xx, zz, y).start()

    def launch_piece(xx):
        @pl.when(z < zs - 1)
        def _():
            dens_z(True, xx, z).start()

        @pl.when(z > 0)
        def _():
            dens_z(False, xx, z).start()

        spread_piece(xx, z)

    local.wait()
    launch_piece(x)
    lax.fori_loop(1, per, begin_far, 0)
    for e in range(1, xs):
        dens_x(e).wait_recv()
        launch_piece(x_at(xs - e))
    lax.fori_loop(0, per, begin_near, 0)

    pair_copy.wait()
    counts_copy.wait()

    base, start = 0, 0
    for m in range(nblk):
        tall_here = (counts_ref[m] + 15) // 16
        lanes = counts_ref[pair_ref[0, m]]
        for j in range(1, neigh):
            lanes = lanes + counts_ref[pair_ref[j, m]]
        wide_here = (lanes + bs - 1) // bs
        if m % chip_blocks == 0:
            base = 0
        tiles_ref[m] = tall_here
        width_ref[m] = wide_here
        base_ref[m] = base
        start_ref[m] = start
        start = start + counts_ref[m]
        base = base + tall_here * wide_here

    def take_tile(k, carry):
        mm = 0
        for q in range(1, chip_blocks):
            mm = mm + jnp.where(k >= base_ref[x * chip_blocks + q], 1, 0)
        at = k - base_ref[x * chip_blocks + mm]
        w = width_ref[x * chip_blocks + mm]
        down = 0
        for q in range(1, tall):
            down = down + jnp.where(at >= q * w, 1, 0)
        along = at - down * w
        take_ref[k] = jnp.where(along < w, (mm * neigh + along) * tall + down, 0)
        return carry

    lax.fori_loop(0, cap, take_tile, 0)

    def fill_pack(mm, carry):
        m = x * chip_blocks + mm
        slot = lax.broadcasted_iota(jnp.int32, (bs, 1), 0)
        place = lax.broadcasted_iota(jnp.int32, (bs, span), 1)
        at = 0
        for j in range(neigh):
            count = counts_ref[pair_ref[j, m]]
            goal = jnp.where(slot < count, slot + at, -1)
            pack[mm, j * bs:(j + 1) * bs, :] = jnp.where(goal == place, 1.0, 0.0).astype(pack.dtype)
            at = at + count
        return carry

    lax.fori_loop(0, chip_blocks, fill_pack, 0)

    def emit(i, carry):
        for e in range(1, xs):
            own_copy(e, i).wait()
            core_copy(e, i).wait_recv()

            def squeeze(mm, carry):
                left = jnp.concatenate([raw[e, i, mm, j] for j in range(neigh)], axis=1)
                close = jnp.dot(left, pack[mm], preferred_element_type=jnp.float32).astype(stage.dtype)
                for j in range(neigh):
                    stage[pl.ds((mm * neigh + j) * tall, tall)] = close[:, j * bs:(j + 1) * bs].reshape(tall, 16, bs)
                return carry

            lax.fori_loop(0, chip_blocks, squeeze, 0)

            def move(k, carry):
                for q in range(4):
                    outbox[e - 1, i, k * 4 + q] = stage[take_ref[k * 4 + q]]
                return carry

            lax.fori_loop(0, cap // 4, move, 0)
            x_copy(e, i).start()
        return carry


    def hop(h, carry):
        def pieces(k, carry):
            xx = x_at(k)

            @pl.when(z - h >= 0)
            def _():
                dens_z(True, xx, z - h).wait_recv()

                @pl.when(z < zs - 1)
                def _():
                    dens_z(True, xx, z - h).start()

                spread_piece(xx, z - h)

            @pl.when(z + h < zs)
            def _():
                dens_z(False, xx, z + h).wait_recv()

                @pl.when(z > 0)
                def _():
                    dens_z(False, xx, z + h).start()

                spread_piece(xx, z + h)

            return carry

        lax.fori_loop(0, xs, pieces, 0)
        from_y(h - 1)
        return carry

    def from_y(h):
        def pieces(k, carry):
            xx = x_at(k)

            def turn(zz):
                for e in range(1, ys):
                    dens_y(e, xx, zz).wait_recv()
                    dens_c(xx, zz, lax.rem(y + ys - e, ys)).start()

            @pl.when(z - h >= 0)
            def _():
                turn(z - h)

            @pl.when((z + h < zs) & (h > 0))
            def _():
                turn(z + h)

            return carry

        lax.fori_loop(0, xs, pieces, 0)

    total[...] = jnp.zeros_like(total)

    def fill_place(m, carry):
        slot = lax.broadcasted_iota(jnp.int32, (bs, 1), 0)
        spot = lax.broadcasted_iota(jnp.int32, (bs, live), 1)
        for j in range(neigh):
            b = pair_ref[j, m]
            goal = jnp.where(slot < counts_ref[b], slot + start_ref[b], -1)
            place[m, j * bs:(j + 1) * bs, :] = jnp.where(goal == spot, 1.0, 0.0).astype(place.dtype)
        return carry

    def fill_far(k, carry):
        m = lax.rem(x * chip_blocks + chip_blocks + k, nblk)
        spot = lax.broadcasted_iota(jnp.int32, (bs, live), 1)
        for q in range(neigh):
            slot = lax.broadcasted_iota(jnp.int32, (bs, 1), 0) + q * bs
            goal = jnp.full((bs, 1), -1, jnp.int32)
            at = 0
            for j in range(neigh):
                b = pair_ref[j, m]
                inside = (slot >= at) & (slot < at + counts_ref[b])
                goal = jnp.where(inside, slot - at + start_ref[b], goal)
                at = at + counts_ref[b]
            place[nblk + k, q * bs:(q + 1) * bs, :] = jnp.where(goal == spot, 1.0, 0.0).astype(place.dtype)
            for down in range(tall):
                inside = (q < width_ref[m]) & (down < tiles_ref[m])
                give_ref[(k * neigh + q) * tall + down] = jnp.where(
                    inside, base_ref[m] + down * width_ref[m] + q, 0
                )
        return carry

    def fill_lift(q, carry):
        spot = lax.broadcasted_iota(jnp.int32, (bs, bs), 0) + q * bs
        slot = lax.broadcasted_iota(jnp.int32, (1, bs), 1)
        for b in range(nblk):
            goal = jnp.where(slot < counts_ref[b], slot + start_ref[b], -1)
            lift[pl.ds(pl.multiple_of(q * bs, bs), bs), b * bs:(b + 1) * bs] = jnp.where(
                goal == spot, 1.0, 0.0
            ).astype(lift.dtype)
        return carry

    def put_wide(m, left, which):
        wide[pl.ds(pl.multiple_of(m * bs, bs), bs), :] = jnp.dot(
            left, place[which], preferred_element_type=jnp.float32
        ).astype(wide.dtype)

    def take_near(i):
        own_copy(0, i).wait()
        core_copy(0, i).wait_recv()

        def put(mm, carry):
            m = x * chip_blocks + mm
            put_wide(m, jnp.concatenate([raw[0, i, mm, j] for j in range(neigh)], axis=1), m)
            return carry

        lax.fori_loop(0, chip_blocks, put, 0)

    def take_far(i):
        for r in range(xs - 1):
            x_copy(xs - 1 - r, i).wait_recv()
            arrived[...] = inbox[r, i]

            def spread(mm, carry):
                for q in range(neigh * tall):
                    stage[mm * neigh * tall + q] = arrived[give_ref[(r * chip_blocks + mm) * neigh * tall + q]]
                close = jnp.concatenate(
                    [stage[pl.ds((mm * neigh + j) * tall, tall)].reshape(bs, bs) for j in range(neigh)], axis=1
                )
                put_wide(x_at(r + 1) * chip_blocks + mm, close, nblk + r * chip_blocks + mm)
                return carry

            lax.fori_loop(0, chip_blocks, spread, 0)

    def take_plain():
        for r in range(xs - 1):
            plain_arrival(r, 0).wait_recv()
            plain_arrival(r, 1).wait_recv()

            def put(mm, carry):
                m = x_at(r + 1) * chip_blocks + mm
                put_wide(m, jnp.concatenate([direct[r, mm, j] for j in range(neigh)], axis=1), m)
                return carry

            lax.fori_loop(0, chip_blocks, put, 0)

    hop(1, 0)
    lax.fori_loop(1, 2, emit, 0)
    lax.fori_loop(0, live // bs, fill_lift, 0)
    def hop_and_emit(h, carry):
        hop(h, carry)
        lax.fori_loop(jnp.minimum(h, per), jnp.minimum(h + 1, per), emit, 0)
        return carry

    lax.fori_loop(2, zs, hop_and_emit, 0)
    lax.fori_loop(0, nblk, fill_place, 0)
    from_y(zs - 1)
    lax.fori_loop(0, (xs - 1) * chip_blocks, fill_far, 0)
    take_near(0)
    take_plain()
    lax.fori_loop(min(zs, per), per, emit, 0)

    def settle(zz, carry):
        for xx in range(xs):
            for yy in range(ys):
                dens_c(xx, zz, yy).wait()
            for e in range(1, ys):
                dens_y(e, xx, zz).wait_send()

            @pl.when((z < zs - 1) & (zz <= z))
            def _():
                dens_z(True, xx, zz).wait_send()

            @pl.when((z > 0) & (zz >= z))
            def _():
                dens_z(False, xx, zz).wait_send()

        return carry

    lax.fori_loop(0, zs, settle, 0)
    for e in range(1, xs):
        dens_x(e).wait_send()

    lane = lax.broadcasted_iota(jnp.int32, (1, bs), 1)
    col_live = jnp.concatenate(
        [jnp.where(lane < counts_ref[b], 1.0, 0.0).astype(jnp.float32) for b in range(nblk)], axis=1
    )

    side = live // 2
    part_cols = min(nbf, 512)

    def fill_near(g, carry):
        at = at_rows(g * group, group)
        for k in range(nbf // part_cols):
            lo = k * part_cols
            found = jnp.dot(lift[at, :], dens[:, lo:lo + part_cols], preferred_element_type=jnp.float32)
            near[at, lo:lo + part_cols] = (found * col_live[:, lo:lo + part_cols]).astype(near.dtype)
        return carry

    def at_rows(first, count):
        return pl.ds(pl.multiple_of(first, 16), count)

    lax.fori_loop(0, live // group, fill_near, 0)

    deep = chip_blocks * bs

    def first_half(first, count):
        at = at_rows(first, count)
        for k in range(nbf // part_cols):
            lo = k * part_cols
            half[at, lo:lo + part_cols] = jnp.dot(
                wide[at, :], near[:, lo:lo + part_cols], preferred_element_type=jnp.float32
            ).astype(half.dtype)

    def second_half(first, count):
        at = at_rows(first, count)
        for lo in range(0, live, part_cols):
            hi = min(lo + part_cols, live)
            total[at, lo:hi] += jnp.dot(half[at, :], wide[:, lo:hi], preferred_element_type=jnp.float32)

    def half_cols(h):
        return slice(h * side, (h + 1) * side)

    def product(g, h):
        at = at_rows(g * group, group)
        total[at, half_cols(h)] += jnp.dot(half[at, :], wide[:, half_cols(h)], preferred_element_type=jnp.float32)

    def one(i, carry):
        def part(xx, carry):
            first_half(xx * deep, deep)
            second_half(xx * deep, deep)
            return carry

        lax.fori_loop(0, xs, part, 0)

        take_near(i + 1)

        @pl.when(i < per - 2)
        def _():
            take_far(i + 1)

        return carry

    lax.fori_loop(0, per - 1, one, 0)

    counter[0] = 0
    ksems = (k_send, k_recv)
    sends = []

    def send_to(src, dst, device):
        cp = remote(src, dst, device, ksems)
        cp.start()
        sends.append(cp)
        return cp

    def part_product(g, q, h):
        at = at_rows(g * group, group)
        qt = at_rows(q * deep, deep)
        qc = pl.ds(pl.multiple_of(q * deep, 128), deep)
        total[at, half_cols(h)] += jnp.dot(
            half[at, qc], wide[qt, half_cols(h)], preferred_element_type=jnp.float32
        )

    def final(e, carry):
        @pl.when(e == 1)
        def _():
            take_far(per - 1)

        def turn(core, carry):
            first_half((x_at(e) * 2 + core) * group, group)

            @pl.when(e == 0)
            def _():
                part_product(x * 2 + core, x, 0)
                part_product(x * 2 + core, x, 1)

            return carry

        lax.fori_loop(0, 2, turn, 0)
        return carry

    lax.fori_loop(0, xs, final, 0)

    def last_product(e, core, h):
        if e:
            product(x_at(e) * 2 + core, h)
        else:
            for f in range(1, xs):
                part_product(x * 2 + core, x_at(f), h)

    left, right = slice(0, side), slice(side, live)

    def y_at(e):
        return lax.rem(y + e, ys)

    core_left, core_right = {}, {}
    for e in list(range(1, xs)) + [0]:
        last_product(e, other, 0)
        last_product(e, other, 1)
        for store, part in ((core_left, left), (core_right, right)):
            store[e] = send_to(
                total.at[at_rows((x_at(e) * 2 + other) * group, group), part],
                from_core.at[e * group:(e + 1) * group, part],
                sibling,
            )

    def core_sum(e, row, count, part):
        return (
            total[at_rows((x_at(e) * 2 + c) * group + row, count), part]
            + from_core[at_rows(e * group + row, count), part]
        )

    zr = zs * rows
    left_x = {}
    for e in range(1, xs):
        last_product(e, c, 0)
        core_left[e].wait_recv()
        for f in list(range(1, ys)) + [0]:
            lo = (e - 1) * group + f * zr
            def pour(zz, carry):
                send[at_rows(lo + zz * rows, rows), left] = core_sum(
                    e, (zz * ys + y_at(f)) * rows, rows, left
                ).astype(send.dtype)
                return carry

            lax.fori_loop(0, zs, pour, 0)
            left_x[e, f] = send_to(
                send.at[lo:lo + zr, left], first_x.at[lo:lo + zr, :], (x_at(e) * 2 + c, u)
            )
    right_y = {}
    for e in list(range(1, xs)) + [0]:
        last_product(e, c, 1)
        core_right[e].wait_recv()
        for f in range(1, ys):
            lo = ((f - 1) * xs + e) * zr
            to = (f - 1) * xs * zr + x_at(e) * zr
            def pour(zz, carry):
                send[at_rows(lo + zz * rows, rows), right] = core_sum(
                    e, (zz * ys + y_at(f)) * rows, rows, right
                ).astype(send.dtype)
                return carry

            lax.fori_loop(0, zs, pour, 0)
            right_y[f, e] = send_to(
                send.at[lo:lo + zr, right], second_y.at[at_rows(to, zr), :], (t, y_peer(f))
            )
    last_product(0, c, 0)
    core_left[0].wait_recv()

    def left_after_x(zz, f):
        value = core_sum(0, (zz * ys + y_at(f)) * rows, rows, left)
        for e in range(xs - 1):
            row = e * group + f * zr + zz * rows
            value = value + first_x[at_rows(row, rows), :].astype(jnp.float32)
        return value

    stage = max((xs - 1) * group, (ys - 1) * xs * zr)
    left_y = []
    for f in range(1, ys):
        lo = stage + (f - 1) * zr
        for e in range(1, xs):
            left_x[e, f].wait_recv()
        def pour(zz, carry):
            send[at_rows(lo + zz * rows, rows), left] = left_after_x(zz, f).astype(send.dtype)
            return carry

        lax.fori_loop(0, zs, pour, 0)
        left_y.append(send_to(
            send.at[lo:lo + zr, left], first_y.at[(f - 1) * zr:f * zr, :], (t, y_peer(f))
        ))

    def right_after_y(e, zz):
        value = core_sum(e, (zz * ys + y) * rows, rows, right)
        for f in range(ys - 1):
            row = f * xs * zr + x_at(e) * zr + zz * rows
            value = value + second_y[at_rows(row, rows), :].astype(jnp.float32)
        return value

    right_x = []
    for e in range(1, xs):
        lo = stage + (e - 1) * zr
        for f in range(1, ys):
            right_y[f, e].wait_recv()
        def pour(zz, carry):
            send[at_rows(lo + zz * rows, rows), right] = right_after_y(e, zz).astype(send.dtype)
            return carry

        lax.fori_loop(0, zs, pour, 0)
        right_x.append(send_to(
            send.at[lo:lo + zr, right], second_x.at[(e - 1) * zr:e * zr, :], (x_at(e) * 2 + c, u)
        ))

    def left_after_y(zz):
        value = left_after_x(zz, 0)
        for f in range(ys - 1):
            value = value + first_y[at_rows(f * zr + zz * rows, rows), :].astype(jnp.float32)
        return value

    def right_after_x(zz):
        value = right_after_y(0, zz)
        for e in range(xs - 1):
            value = value + second_x[at_rows(e * zr + zz * rows, rows), :].astype(jnp.float32)
        return value

    stage = stage + max(xs - 1, ys - 1) * zr
    ends = []
    for waits, after, into, part in (
        (left_y, left_after_y, first_z, left), (right_x, right_after_x, second_z, right)
    ):
        for cp in waits:
            cp.wait_recv()
        if part == right:
            for f in range(1, ys):
                right_y[f, 0].wait_recv()
        else:
            for e in range(1, xs):
                left_x[e, 0].wait_recv()
        arrivals = []
        for e in range(1, zs):
            lo = stage + (e - 1) * rows
            send[lo:lo + rows, part] = after(lax.rem(z + e, zs)).astype(send.dtype)
            arrivals.append(send_to(
                send.at[lo:lo + rows, part], into.at[(e - 1) * rows:e * rows, :], (t, z_peer(e))
            ))
        ends.append((arrivals, after, into, part))
    block = mine // bs
    slot = lax.broadcasted_iota(jnp.int32, (rows, 1), 0) + mine % bs
    row_live = jnp.where(slot < counts_ref[block], 1.0, 0.0).astype(jnp.float32)
    for arrivals, after, into, part in ends:
        value = after(z)
        for e in range(zs - 1):
            arrivals[e].wait_recv()
            value = value + into[e * rows:(e + 1) * rows, :].astype(jnp.float32)
        for k in range(3):
            bits = value.astype(cut.dtype)
            cut[k * rows:(k + 1) * rows, part] = bits
            value = value - bits.astype(jnp.float32)
    whole = jnp.dot(cut[...], lift[...], preferred_element_type=jnp.float32)
    whole = whole[:rows] + whole[rows:2 * rows] + whole[2 * rows:]
    out_ref[...] = whole * row_live
    for cp in sends:
        cp.wait_send()

    def finish(i, carry):
        core_copy(0, i).wait_send()

        @pl.when(i > 0)
        def _():
            for e in range(1, xs):
                core_copy(e, i).wait_send()
                x_copy(e, i).wait_send()

        return carry

    lax.fori_loop(0, per, finish, 0)
    for e in range(1, xs):
        plain_copy(e, 0).wait_send()
        plain_copy(e, 1).wait_send()


def packed_caps(chip_blocks, neigh, bs):
    full = chip_blocks * neigh * (bs // 16)
    return [full * k // 32 // 4 * 4 for k in (23, 25, 28)] + [full]


def packed_scratch(cap, atoms, aux, xs, ys, zs, per, nblk, neigh, bs, rows):
    nbf, chip_blocks, group = nblk * bs, nblk // xs, aux * rows
    live = nbf * 3 // 4
    side, zr, span, tall = live // 2, zs * rows, neigh * bs, bs // 16
    n_k = 2 * (xs + (xs - 1) + (ys - 1) + (zs - 1)) + 2 * (xs - 1) * (ys - 1)
    send_rows = max((xs - 1) * group, (ys - 1) * xs * zr) + max(xs - 1, ys - 1) * zr + zr
    vmem, smem, dma = pltpu.VMEM, pltpu.SMEM, pltpu.SemaphoreType.DMA
    bf16, f32 = jnp.bfloat16, jnp.float32
    far = max(xs - 1, 1)
    return [
        smem((neigh, nblk), jnp.int32),
        smem((nblk,), jnp.int32),
        smem((nblk,), jnp.int32),
        smem((nblk,), jnp.int32),
        smem((nblk,), jnp.int32),
        smem((nblk,), jnp.int32),
        smem((cap,), jnp.int32),
        smem((far * chip_blocks * neigh * tall,), jnp.int32),
        vmem((nbf, nbf), bf16),
        vmem((xs, per, chip_blocks, neigh, bs, bs), bf16),
        vmem((far, chip_blocks, neigh, bs, bs), bf16),
        vmem((far, per, cap, 16, bs), bf16),
        vmem((far, per, cap, 16, bs), bf16),
        vmem((chip_blocks * neigh * tall, 16, bs), bf16),
        vmem((cap, 16, bs), bf16),
        vmem((chip_blocks, span, span), bf16),
        vmem((nblk + far * chip_blocks, span, live), bf16),
        vmem((live, nbf), bf16),
        vmem((live, nbf), bf16),
        vmem((nbf, live), bf16),
        vmem((nbf, nbf), bf16),
        vmem((send_rows, live), bf16),
        vmem((nbf, live), f32),
        vmem((xs * group, live), f32),
        vmem((far * group, side), bf16),
        vmem((max(ys - 1, 1) * zr, side), bf16),
        vmem((max(zs - 1, 1) * rows, side), bf16),
        vmem((max(ys - 1, 1) * xs * zr, side), bf16),
        vmem((far * zr, side), bf16),
        vmem((max(zs - 1, 1) * rows, side), bf16),
        vmem((3 * rows, live), bf16),
        dma((xs, per)),
        dma,
        dma,
        dma,
        dma((xs, per)),
        dma((xs, per)),
        dma((far, 2)),
        dma((far, 2)),
        dma((far, per)),
        dma((far, per)),
        dma((far,)),
        dma((far,)),
        dma((2, zs, xs)),
        dma((zs, xs)),
        dma((zs, xs, max(ys - 1, 1))),
        dma((zs, xs, max(ys - 1, 1))),
        dma((zs, ys, xs)),
        dma((zs, ys, xs)),
        dma((n_k,)),
        dma((n_k,)),
    ]


VMEM_BYTES = 67043328


def packed_call(which, cap, sizes, three_index, density, pair_blocks, basis_counts):
    atoms, aux, xs, ys, zs = sizes[:5]
    rows, nbf = density.shape
    anywhere = pl.BlockSpec(memory_space=pl.ANY)
    return pl.pallas_call(
        functools.partial(packed_kernel, cap, atoms, aux, xs, ys, zs),
        out_shape=jax.ShapeDtypeStruct((rows, nbf), jnp.float32),
        in_specs=[anywhere] * 4,
        out_specs=pl.BlockSpec(memory_space=pltpu.VMEM),
        scratch_shapes=packed_scratch(cap, *sizes),
        compiler_params=pltpu.CompilerParams(
            collective_id=which, has_side_effects=True, vmem_limit_bytes=VMEM_BYTES
        ),
    )(pair_blocks.T, basis_counts, three_index, density)


def per_device(atoms, aux, three_index, density, pair_blocks, basis_counts):
    aux_here, own_blocks, neigh, bs, _ = three_index.shape
    rows, nbf = density.shape
    nblk = nbf // bs
    xs = atoms // 2
    ys = xs if aux % xs == 0 else 1
    zs = aux // ys
    per = aux_here // atoms
    sizes = (atoms, aux, xs, ys, zs, per, nblk, neigh, bs, rows)
    caps = packed_caps(nblk // xs, neigh, bs)
    need = sum(
        math.prod(ref.shape) * jnp.dtype(ref.dtype).itemsize
        for ref in packed_scratch(caps[-1], *sizes) if getattr(ref, 'memory_space', None) == pltpu.VMEM
    )
    if per < 2 or nbf * 3 // 4 % (aux * rows) or nbf * 3 % (8 * bs) or need + 2 * rows * nbf * 4 > VMEM_BYTES - 2**21:
        return plain_device(atoms, aux, three_index, density, pair_blocks, basis_counts)
    hit = pair_blocks[:, :, None] == jnp.arange(nblk)[None, None, :]
    lanes = jnp.sum(jnp.where(hit, basis_counts[None, None, :], 0), axis=(1, 2))
    tiles = ((basis_counts + 15) >> 4) * ((lanes + bs - 1) // bs)
    chip = functools.reduce(jnp.maximum, [jnp.sum(part) for part in jnp.split(tiles, xs)])
    choice = sum((chip > cap).astype(jnp.int32) for cap in caps[:-1])
    branches = [functools.partial(packed_call, k, cap, sizes) for k, cap in enumerate(caps)]
    return lax.switch(choice, branches, three_index, density, pair_blocks, basis_counts)


def solution(mesh):
    in_specs = (P("aux", "atom", None, None, None), P(("atom", "aux"), None), P(), P())
    out_specs = P(("atom", "aux"), None)
    return jax.shard_map(
        functools.partial(per_device, mesh.shape["atom"], mesh.shape["aux"]),
        mesh=mesh, in_specs=in_specs, out_specs=out_specs, check_vma=False,
    )
```

```python
import functools
import math

import jax
import jax.numpy as jnp
from jax import lax
from jax.experimental import pallas as pl
from jax.experimental.pallas import tpu as pltpu
from jax.sharding import PartitionSpec as P

MESH = pl.DeviceIdType.MESH


def kernel(
    atoms, aux, xs, ys, zs,
    pair_hbm, counts_hbm, tensor_ref, piece_ref, out_ref,
    pair_ref, counts_ref, dens, tens, wide, half, send, total, from_core,
    first_x, first_y, first_z, second_y, second_x, second_z,
    own_sem, piece_sem, pair_sem, counts_sem, t_send, t_recv, d_send, d_recv, k_send, k_recv,
):
    per, nblk, neigh, bs = tens.shape[0], tens.shape[1], tens.shape[2], tens.shape[3]
    nbf = total.shape[1]
    own_blocks = nblk // atoms
    rows = piece_ref.shape[0]
    group = aux * rows
    t = lax.axis_index("atom")
    u = lax.axis_index("aux")
    x, c = t // 2, t % 2
    z, y = u // ys, u % ys

    pair_copy = pltpu.make_async_copy(pair_hbm, pair_ref, pair_sem)
    counts_copy = pltpu.make_async_copy(counts_hbm, counts_ref, counts_sem)
    pair_copy.start()
    counts_copy.start()

    def atom_peer(d):
        return lax.rem(t + d, atoms)

    def x_peer(e):
        return lax.rem(x + e, xs) * 2 + c

    def y_peer(e):
        return z * ys + lax.rem(y + e, ys)

    def z_peer(e):
        return lax.rem(z + e, zs) * ys + y

    barrier = pltpu.get_barrier_semaphore()
    for d in range(1, atoms):
        pl.semaphore_signal(barrier, inc=1, device_id=(atom_peer(d), u), device_id_type=MESH)
    for e in range(1, ys):
        pl.semaphore_signal(barrier, inc=1, device_id=(t, y_peer(e)), device_id_type=MESH)
    for e in range(1, zs):
        pl.semaphore_signal(barrier, inc=1, device_id=(t, z_peer(e)), device_id_type=MESH)
    pl.semaphore_wait(barrier, (atoms - 1) + (ys - 1) + (zs - 1))

    counter = [0]

    def remote(src, dst, device, sems):
        k = counter[0]
        counter[0] += 1
        return pltpu.make_async_remote_copy(
            src_ref=src, dst_ref=dst, send_sem=sems[0].at[k], recv_sem=sems[1].at[k],
            device_id=device, device_id_type=MESH,
        )

    dsems = (d_send, d_recv)

    def dens_rows(first, count):
        return dens.at[first // bs, pl.ds(pl.multiple_of(first % bs, 16), count), :]

    mine = (t * aux + u) * rows
    local = pltpu.make_async_copy(piece_ref, dens_rows(mine, rows), piece_sem)
    local.start()
    over_x = []
    for e in range(1, xs):
        cp = remote(piece_ref, dens_rows(mine, rows), (x_peer(e), u), dsems)
        cp.start()
        over_x.append(cp)

    def own_copy(i):
        return pltpu.make_async_copy(
            tensor_ref.at[t * per + i], tens.at[i, pl.ds(t * own_blocks, own_blocks)], own_sem.at[i]
        )

    def t_copy(i, d):
        to = atom_peer(d)
        return pltpu.make_async_remote_copy(
            src_ref=tensor_ref.at[to * per + i],
            dst_ref=tens.at[i, pl.ds(t * own_blocks, own_blocks)],
            send_sem=t_send.at[i, d - 1],
            recv_sem=t_recv.at[i, d - 1],
            device_id=(to, u),
            device_id_type=MESH,
        )

    order = list(range(1, atoms, 2)) + list(range(2, atoms, 2))

    def begin(i, carry):
        for d in order:
            t_copy(i, d).start()
        own_copy(i).start()
        return carry

    lax.fori_loop(0, per, begin, 0)

    local.wait()
    for cp in over_x:
        cp.wait()
    over_y = []
    for xx in range(xs):
        first = ((xx * 2 + c) * aux + u) * rows
        for e in range(1, ys):
            cp = remote(dens_rows(first, rows), dens_rows(first, rows), (t, y_peer(e)), dsems)
            cp.start()
            over_y.append(cp)
    total[...] = jnp.zeros_like(total)
    for cp in over_y:
        cp.wait()
    over_z = []
    for xx in range(xs):
        first = ((xx * 2 + c) * aux + z * ys) * rows
        for e in range(1, zs):
            cp = remote(dens_rows(first, ys * rows), dens_rows(first, ys * rows), (t, z_peer(e)), dsems)
            cp.start()
            over_z.append(cp)
    for cp in over_z:
        cp.wait()
    over_c = []
    for xx in range(xs):
        blocks = dens.at[pl.ds((xx * 2 + c) * own_blocks, own_blocks)]
        cp = remote(blocks, blocks, (x * 2 + (1 - c), u), dsems)
        cp.start()
        over_c.append(cp)
    for cp in over_c:
        cp.wait()

    pair_copy.wait()
    counts_copy.wait()
    lane = lax.broadcasted_iota(jnp.int32, (1, bs), 1)
    col_live = jnp.concatenate(
        [jnp.where(lane < counts_ref[b], 1.0, 0.0).astype(jnp.float32) for b in range(nblk)], axis=1
    )

    def mask_rows(b, carry):
        slot = lax.broadcasted_iota(jnp.int32, (bs, 1), 0)
        row_live = jnp.where(slot < counts_ref[b], 1.0, 0.0).astype(jnp.float32)
        dens[b] = (dens[b].astype(jnp.float32) * row_live * col_live).astype(dens.dtype)
        return carry

    lax.fori_loop(0, nblk, mask_rows, 0)

    side = nbf // 2
    cols = min(side, 512)

    def at_rows(first, count):
        return pl.ds(pl.multiple_of(first, 16), count)

    def arrive(i):
        own_copy(i).wait()
        for d in range(1, atoms):
            t_copy(i, d).wait_recv()

    def first_half(i, first, count):
        def block_row(k, carry):
            m = first + k
            left = jnp.concatenate([tens[i, m, j] for j in range(neigh)], axis=1)
            right = jnp.concatenate([dens[pair_ref[j, m]] for j in range(neigh)], axis=0)
            h = jnp.dot(left, right, preferred_element_type=jnp.float32)
            at = pl.ds(pl.multiple_of(m * bs, bs), bs)
            half[at, :] = h.astype(half.dtype)
            for n in range(nblk):
                block = jnp.zeros((bs, bs), wide.dtype)
                for j in range(neigh):
                    block = jnp.where(pair_ref[j, m] == n, tens[i, m, j], block)
                wide[at, n * bs:(n + 1) * bs] = block
            return carry

        lax.fori_loop(0, count, block_row, 0)

    def product(g, h):
        at = at_rows(g * group, group)
        for k in range(side // cols):
            lo = h * side + k * cols
            total[at, lo:lo + cols] += jnp.dot(
                half[at, :], wide[:, lo:lo + cols], preferred_element_type=jnp.float32
            )

    def one(i, carry):
        arrive(i)
        first_half(i, 0, nblk)

        def second_half(g, carry):
            product(g, 0)
            product(g, 1)
            return carry

        lax.fori_loop(0, atoms, second_half, 0)
        return carry

    lax.fori_loop(0, per - 1, one, 0)

    counter[0] = 0
    ksems = (k_send, k_recv)
    sends = []

    def send_to(src, dst, device):
        cp = remote(src, dst, device, ksems)
        cp.start()
        sends.append(cp)
        return cp

    other = 1 - c
    sibling = (x * 2 + other, u)
    final = per - 1
    own_copy(final).wait()
    for d in order[:-1]:
        t_copy(final, d).wait_recv()
    late = lax.rem(t + atoms - order[-1], atoms)

    def part_product(g, q, h):
        at, qt = at_rows(g * group, group), at_rows(q * group, group)
        qc = pl.ds(pl.multiple_of(q * group, 128), group)
        for k in range(side // cols):
            lo = h * side + k * cols
            total[at, lo:lo + cols] += jnp.dot(
                half[at, qc], wide[qt, lo:lo + cols], preferred_element_type=jnp.float32
            )

    def early_rows(k, carry):
        first_half(final, lax.rem(late + k, atoms) * own_blocks, own_blocks)
        return carry

    lax.fori_loop(1, atoms, early_rows, 0)

    def early_products(k, carry):
        g = (k // (atoms - 1)) * 2 + other
        q = lax.rem(late + 1 + k % (atoms - 1), atoms)
        part_product(g, q, 0)
        part_product(g, q, 1)
        return carry

    lax.fori_loop(0, xs * (atoms - 1), early_products, 0)
    t_copy(final, order[-1]).wait_recv()
    first_half(final, late * own_blocks, own_blocks)

    def last_product(e, core, h):
        if core is c:
            product(x_at(e) * 2 + c, h)
        else:
            part_product(x_at(e) * 2 + other, late, h)

    left, right = slice(0, side), slice(side, nbf)

    def x_at(e):
        return lax.rem(x + e, xs)

    def y_at(e):
        return lax.rem(y + e, ys)

    core_left, core_right = {}, {}
    for e in list(range(1, xs)) + [0]:
        last_product(e, other, 0)
        last_product(e, other, 1)
        for store, part in ((core_left, left), (core_right, right)):
            store[e] = send_to(
                total.at[at_rows((x_at(e) * 2 + other) * group, group), part],
                from_core.at[e * group:(e + 1) * group, part],
                sibling,
            )

    def core_sum(e, row, count, part):
        return (
            total[at_rows((x_at(e) * 2 + c) * group + row, count), part]
            + from_core[at_rows(e * group + row, count), part]
        )

    zr = zs * rows
    left_x = {}
    for e in range(1, xs):
        last_product(e, c, 0)
        core_left[e].wait_recv()
        for f in list(range(1, ys)) + [0]:
            lo = (e - 1) * group + f * zr
            for zz in range(zs):
                send[lo + zz * rows:lo + (zz + 1) * rows, left] = core_sum(
                    e, (zz * ys + y_at(f)) * rows, rows, left
                ).astype(send.dtype)
            left_x[e, f] = send_to(
                send.at[lo:lo + zr, left], first_x.at[lo:lo + zr, :], (x_at(e) * 2 + c, u)
            )
    right_y = {}
    for e in list(range(1, xs)) + [0]:
        last_product(e, c, 1)
        core_right[e].wait_recv()
        for f in range(1, ys):
            lo = ((f - 1) * xs + e) * zr
            to = (f - 1) * xs * zr + x_at(e) * zr
            for zz in range(zs):
                send[lo + zz * rows:lo + (zz + 1) * rows, right] = core_sum(
                    e, (zz * ys + y_at(f)) * rows, rows, right
                ).astype(send.dtype)
            right_y[f, e] = send_to(
                send.at[lo:lo + zr, right], second_y.at[at_rows(to, zr), :], (t, y_peer(f))
            )
    last_product(0, c, 0)
    core_left[0].wait_recv()

    def left_after_x(zz, f):
        value = core_sum(0, (zz * ys + y_at(f)) * rows, rows, left)
        for e in range(xs - 1):
            row = e * group + f * zr + zz * rows
            value = value + first_x[at_rows(row, rows), :].astype(jnp.float32)
        return value

    stage = max((xs - 1) * group, (ys - 1) * xs * zr)
    left_y = []
    for f in range(1, ys):
        lo = stage + (f - 1) * zr
        for e in range(1, xs):
            left_x[e, f].wait_recv()
        for zz in range(zs):
            send[lo + zz * rows:lo + (zz + 1) * rows, left] = left_after_x(zz, f).astype(send.dtype)
        left_y.append(send_to(
            send.at[lo:lo + zr, left], first_y.at[(f - 1) * zr:f * zr, :], (t, y_peer(f))
        ))

    def right_after_y(e, zz):
        value = core_sum(e, (zz * ys + y) * rows, rows, right)
        for f in range(ys - 1):
            row = f * xs * zr + x_at(e) * zr + zz * rows
            value = value + second_y[at_rows(row, rows), :].astype(jnp.float32)
        return value

    right_x = []
    for e in range(1, xs):
        lo = stage + (e - 1) * zr
        for f in range(1, ys):
            right_y[f, e].wait_recv()
        for zz in range(zs):
            send[lo + zz * rows:lo + (zz + 1) * rows, right] = right_after_y(e, zz).astype(send.dtype)
        right_x.append(send_to(
            send.at[lo:lo + zr, right], second_x.at[(e - 1) * zr:e * zr, :], (x_at(e) * 2 + c, u)
        ))

    def left_after_y(zz):
        value = left_after_x(zz, 0)
        for f in range(ys - 1):
            value = value + first_y[at_rows(f * zr + zz * rows, rows), :].astype(jnp.float32)
        return value

    def right_after_x(zz):
        value = right_after_y(0, zz)
        for e in range(xs - 1):
            value = value + second_x[at_rows(e * zr + zz * rows, rows), :].astype(jnp.float32)
        return value

    stage = stage + max(xs - 1, ys - 1) * zr
    ends = []
    for waits, after, into, part in (
        (left_y, left_after_y, first_z, left), (right_x, right_after_x, second_z, right)
    ):
        for cp in waits:
            cp.wait_recv()
        if part == right:
            for f in range(1, ys):
                right_y[f, 0].wait_recv()
        else:
            for e in range(1, xs):
                left_x[e, 0].wait_recv()
        arrivals = []
        for e in range(1, zs):
            lo = stage + (e - 1) * rows
            send[lo:lo + rows, part] = after(lax.rem(z + e, zs)).astype(send.dtype)
            arrivals.append(send_to(
                send.at[lo:lo + rows, part], into.at[(e - 1) * rows:e * rows, :], (t, z_peer(e))
            ))
        ends.append((arrivals, after, into, part))
    block = mine // bs
    slot = lax.broadcasted_iota(jnp.int32, (rows, 1), 0) + mine % bs
    row_live = jnp.where(slot < counts_ref[block], 1.0, 0.0).astype(jnp.float32)
    for arrivals, after, into, part in ends:
        value = after(z)
        for e in range(zs - 1):
            arrivals[e].wait_recv()
            value = value + into[e * rows:(e + 1) * rows, :].astype(jnp.float32)
        out_ref[:, part] = value * row_live * col_live[:, part]
    for cp in sends:
        cp.wait_send()

    def finish(i, carry):
        for d in range(1, atoms):
            t_copy(i, d).wait_send()
        return carry

    lax.fori_loop(0, per, finish, 0)


def plain_device(atoms, aux, three_index, density, pair_blocks, basis_counts):
    aux_here, own_blocks, neigh, bs, _ = three_index.shape
    rows, nbf = density.shape
    nblk = nbf // bs
    xs = atoms // 2
    ys = xs if aux % xs == 0 else 1
    zs = aux // ys
    per = aux_here // atoms
    group = aux * rows
    n_d = (xs - 1) + xs * (ys - 1) + xs * (zs - 1) + xs
    n_k = 2 * (xs + (xs - 1) + (ys - 1) + (zs - 1)) + 2 * (xs - 1) * (ys - 1)
    side = nbf // 2
    zr = zs * rows
    send_rows = max((xs - 1) * group, (ys - 1) * xs * zr) + max(xs - 1, ys - 1) * zr + zr
    vmem, dma = pltpu.VMEM, pltpu.SemaphoreType.DMA
    bf16, f32 = jnp.bfloat16, jnp.float32
    return pl.pallas_call(
        functools.partial(kernel, atoms, aux, xs, ys, zs),
        out_shape=jax.ShapeDtypeStruct((rows, nbf), f32),
        in_specs=[
            pl.BlockSpec(memory_space=pl.ANY),
            pl.BlockSpec(memory_space=pl.ANY),
            pl.BlockSpec(memory_space=pl.ANY),
            pl.BlockSpec(memory_space=pl.ANY),
        ],
        out_specs=pl.BlockSpec(memory_space=pltpu.VMEM),
        scratch_shapes=[
            pltpu.SMEM(pair_blocks.shape[::-1], jnp.int32),
            pltpu.SMEM(basis_counts.shape, jnp.int32),
            vmem((nblk, bs, nbf), bf16),
            vmem((per, nblk, neigh, bs, bs), bf16),
            vmem((nbf, nbf), bf16),
            vmem((nbf, nbf), bf16),
            vmem((send_rows, nbf), bf16),
            vmem((nbf, nbf), f32),
            vmem((xs * group, nbf), f32),
            vmem((max(xs - 1, 1) * group, side), bf16),
            vmem((max(ys - 1, 1) * zs * rows, side), bf16),
            vmem((max(zs - 1, 1) * rows, side), bf16),
            vmem((max(ys - 1, 1) * xs * zs * rows, side), bf16),
            vmem((max(xs - 1, 1) * zs * rows, side), bf16),
            vmem((max(zs - 1, 1) * rows, side), bf16),
            dma((per,)),
            dma,
            dma,
            dma,
            dma((per, atoms - 1)),
            dma((per, atoms - 1)),
            dma((n_d,)),
            dma((n_d,)),
            dma((n_k,)),
            dma((n_k,)),
        ],
        compiler_params=pltpu.CompilerParams(
            collective_id=0, has_side_effects=True, vmem_limit_bytes=67043328
        ),
    )(pair_blocks.T, basis_counts, three_index, density)


def packed_kernel(
    cap, atoms, aux, xs, ys, zs,
    pair_hbm, counts_hbm, tensor_ref, piece_ref, out_ref,
    pair_ref, counts_ref, tiles_ref, width_ref, base_ref, start_ref, take_ref, give_ref,
    dens, raw, direct, outbox, inbox, stage, arrived, pack, place, lift, near,
    wide, half, send, total, from_core,
    first_x, first_y, first_z, second_y, second_x, second_z, cut,
    own_sem, piece_sem, pair_sem, counts_sem, t_send, t_recv, p_send, p_recv, x_send, x_recv, dx_send, dx_recv, dz_send, dz_recv, dy_send, dy_recv,
    dc_send, dc_recv, k_send, k_recv,
):
    per, chip_blocks, neigh, bs = raw.shape[1], raw.shape[2], raw.shape[3], raw.shape[4]
    nbf, live = half.shape[1], total.shape[1]
    nblk = nbf // bs
    own_blocks = nblk // atoms
    rows = piece_ref.shape[0]
    group = aux * rows
    tall = bs // 16
    span = neigh * bs
    t = lax.axis_index("atom")
    u = lax.axis_index("aux")
    x, c = t // 2, t % 2
    z, y = u // ys, u % ys
    other = 1 - c
    sibling = (x * 2 + other, u)

    pair_copy = pltpu.make_async_copy(pair_hbm, pair_ref, pair_sem)
    counts_copy = pltpu.make_async_copy(counts_hbm, counts_ref, counts_sem)
    pair_copy.start()
    counts_copy.start()

    def x_at(e):
        return lax.rem(x + e, xs)

    def x_peer(e):
        return x_at(e) * 2 + c

    def y_peer(e):
        return z * ys + lax.rem(y + e, ys)

    def z_peer(e):
        return lax.rem(z + e, zs) * ys + y

    def own_copy(e, i):
        return pltpu.make_async_copy(
            tensor_ref.at[x_peer(e) * per + i], raw.at[e, i, pl.ds(c * own_blocks, own_blocks)], own_sem.at[e, i]
        )

    def core_copy(e, i):
        return pltpu.make_async_remote_copy(
            src_ref=tensor_ref.at[(x_at(e) * 2 + other) * per + i],
            dst_ref=raw.at[e, i, pl.ds(c * own_blocks, own_blocks)],
            send_sem=t_send.at[e, i], recv_sem=t_recv.at[e, i],
            device_id=sibling, device_id_type=MESH,
        )

    def x_copy(e, i):
        return pltpu.make_async_remote_copy(
            src_ref=outbox.at[e - 1, i], dst_ref=inbox.at[xs - e - 1, i],
            send_sem=x_send.at[e - 1, i], recv_sem=x_recv.at[xs - e - 1, i],
            device_id=(x_peer(e), u), device_id_type=MESH,
        )

    def plain_copy(e, core):
        return pltpu.make_async_remote_copy(
            src_ref=tensor_ref.at[(x_at(e) * 2 + core) * per],
            dst_ref=direct.at[xs - e - 1, pl.ds(c * own_blocks, own_blocks)],
            send_sem=p_send.at[e - 1, core], recv_sem=p_recv.at[xs - e - 1, c],
            device_id=(x_at(e) * 2 + core, u), device_id_type=MESH,
        )

    def plain_arrival(r, core):
        here = direct.at[r, pl.ds(core * own_blocks, own_blocks)]
        return pltpu.make_async_remote_copy(
            src_ref=here, dst_ref=here, send_sem=p_send.at[r, core], recv_sem=p_recv.at[r, core],
            device_id=sibling, device_id_type=MESH,
        )

    def piece(xx, zz, yy):
        first = ((xx * 2 + c) * aux + zz * ys + yy) * rows
        return dens.at[pl.ds(pl.multiple_of(first, 16), rows), :]

    def dens_copy(xx, zz, yy, device, send_sem, recv_sem):
        return pltpu.make_async_remote_copy(
            src_ref=piece(xx, zz, yy), dst_ref=piece(xx, zz, yy), send_sem=send_sem, recv_sem=recv_sem,
            device_id=device, device_id_type=MESH,
        )

    def dens_x(e):
        return pltpu.make_async_remote_copy(
            src_ref=piece_ref, dst_ref=piece(x, z, y), send_sem=dx_send.at[e - 1], recv_sem=dx_recv.at[e - 1],
            device_id=(x_peer(e), u), device_id_type=MESH,
        )

    def dens_z(up, xx, zz):
        to = (z + 1 if up else z - 1) * ys + y
        return dens_copy(xx, zz, y, (t, to), dz_send.at[int(up), zz, xx], dz_recv.at[zz, xx])

    def dens_y(e, xx, zz):
        return dens_copy(xx, zz, y, (t, y_peer(e)), dy_send.at[zz, xx, e - 1], dy_recv.at[zz, xx, e - 1])

    def dens_c(xx, zz, yy):
        return dens_copy(xx, zz, yy, sibling, dc_send.at[zz, yy, xx], dc_recv.at[zz, yy, xx])

    mine = (t * aux + u) * rows
    barrier = pltpu.get_barrier_semaphore()
    pl.semaphore_signal(barrier, inc=1, device_id=sibling, device_id_type=MESH)
    for e in range(1, xs):
        pl.semaphore_signal(barrier, inc=1, device_id=(x_peer(e), u), device_id_type=MESH)
        pl.semaphore_signal(barrier, inc=1, device_id=(x_at(e) * 2 + other, u), device_id_type=MESH)
    for e in range(1, ys):
        pl.semaphore_signal(barrier, inc=1, device_id=(t, y_peer(e)), device_id_type=MESH)
    for e in range(1, zs):
        pl.semaphore_signal(barrier, inc=1, device_id=(t, z_peer(e)), device_id_type=MESH)
    local = pltpu.make_async_copy(piece_ref, piece(x, z, y), piece_sem)
    local.start()
    pl.semaphore_wait(barrier, 1 + 2 * (xs - 1) + (ys - 1) + (zs - 1))

    for e in range(1, xs):
        dens_x(e).start()
    for e in range(1, xs):
        plain_copy(e, 0).start()
        plain_copy(e, 1).start()

    counter = [0]

    def remote(src, dst, device, sems):
        k = counter[0]
        counter[0] += 1
        return pltpu.make_async_remote_copy(
            src_ref=src, dst_ref=dst, send_sem=sems[0].at[k], recv_sem=sems[1].at[k],
            device_id=device, device_id_type=MESH,
        )

    def begin_far(i, carry):
        for e in range(1, xs):
            core_copy(e, i).start()
            own_copy(e, i).start()
        return carry

    def begin_near(i, carry):
        core_copy(0, i).start()
        own_copy(0, i).start()
        return carry

    def spread_piece(xx, zz):
        for e in range(1, ys):
            dens_y(e, xx, zz).start()
        dens_c(xx, zz, y).start()

    def launch_piece(xx):
        @pl.when(z < zs - 1)
        def _():
            dens_z(True, xx, z).start()

        @pl.when(z > 0)
        def _():
            dens_z(False, xx, z).start()

        spread_piece(xx, z)

    local.wait()
    launch_piece(x)
    lax.fori_loop(1, per, begin_far, 0)
    for e in range(1, xs):
        dens_x(e).wait_recv()
        launch_piece(x_at(xs - e))
    lax.fori_loop(0, per, begin_near, 0)

    pair_copy.wait()
    counts_copy.wait()

    base, start = 0, 0
    for m in range(nblk):
        tall_here = (counts_ref[m] + 15) // 16
        lanes = counts_ref[pair_ref[0, m]]
        for j in range(1, neigh):
            lanes = lanes + counts_ref[pair_ref[j, m]]
        wide_here = (lanes + bs - 1) // bs
        if m % chip_blocks == 0:
            base = 0
        tiles_ref[m] = tall_here
        width_ref[m] = wide_here
        base_ref[m] = base
        start_ref[m] = start
        start = start + counts_ref[m]
        base = base + tall_here * wide_here

    def take_tile(k, carry):
        mm = 0
        for q in range(1, chip_blocks):
            mm = mm + jnp.where(k >= base_ref[x * chip_blocks + q], 1, 0)
        at = k - base_ref[x * chip_blocks + mm]
        w = width_ref[x * chip_blocks + mm]
        down = 0
        for q in range(1, tall):
            down = down + jnp.where(at >= q * w, 1, 0)
        along = at - down * w
        take_ref[k] = jnp.where(along < w, (mm * neigh + along) * tall + down, 0)
        return carry

    lax.fori_loop(0, cap, take_tile, 0)

    def fill_pack(mm, carry):
        m = x * chip_blocks + mm
        slot = lax.broadcasted_iota(jnp.int32, (bs, 1), 0)
        place = lax.broadcasted_iota(jnp.int32, (bs, span), 1)
        at = 0
        for j in range(neigh):
            count = counts_ref[pair_ref[j, m]]
            goal = jnp.where(slot < count, slot + at, -1)
            pack[mm, j * bs:(j + 1) * bs, :] = jnp.where(goal == place, 1.0, 0.0).astype(pack.dtype)
            at = at + count
        return carry

    lax.fori_loop(0, chip_blocks, fill_pack, 0)

    def emit(i, carry):
        for e in range(1, xs):
            own_copy(e, i).wait()
            core_copy(e, i).wait_recv()

            def squeeze(mm, carry):
                left = jnp.concatenate([raw[e, i, mm, j] for j in range(neigh)], axis=1)
                close = jnp.dot(left, pack[mm], preferred_element_type=jnp.float32).astype(stage.dtype)
                for j in range(neigh):
                    stage[pl.ds((mm * neigh + j) * tall, tall)] = close[:, j * bs:(j + 1) * bs].reshape(tall, 16, bs)
                return carry

            lax.fori_loop(0, chip_blocks, squeeze, 0)

            def move(k, carry):
                for q in range(4):
                    outbox[e - 1, i, k * 4 + q] = stage[take_ref[k * 4 + q]]
                return carry

            lax.fori_loop(0, cap // 4, move, 0)
            x_copy(e, i).start()
        return carry


    def hop(h, carry):
        def pieces(k, carry):
            xx = x_at(k)

            @pl.when(z - h >= 0)
            def _():
                dens_z(True, xx, z - h).wait_recv()

                @pl.when(z < zs - 1)
                def _():
                    dens_z(True, xx, z - h).start()

                spread_piece(xx, z - h)

            @pl.when(z + h < zs)
            def _():
                dens_z(False, xx, z + h).wait_recv()

                @pl.when(z > 0)
                def _():
                    dens_z(False, xx, z + h).start()

                spread_piece(xx, z + h)

            return carry

        lax.fori_loop(0, xs, pieces, 0)
        from_y(h - 1)
        return carry

    def from_y(h):
        def pieces(k, carry):
            xx = x_at(k)

            def turn(zz):
                for e in range(1, ys):
                    dens_y(e, xx, zz).wait_recv()
                    dens_c(xx, zz, lax.rem(y + ys - e, ys)).start()

            @pl.when(z - h >= 0)
            def _():
                turn(z - h)

            @pl.when((z + h < zs) & (h > 0))
            def _():
                turn(z + h)

            return carry

        lax.fori_loop(0, xs, pieces, 0)

    total[...] = jnp.zeros_like(total)

    def fill_place(m, carry):
        slot = lax.broadcasted_iota(jnp.int32, (bs, 1), 0)
        spot = lax.broadcasted_iota(jnp.int32, (bs, live), 1)
        for j in range(neigh):
            b = pair_ref[j, m]
            goal = jnp.where(slot < counts_ref[b], slot + start_ref[b], -1)
            place[m, j * bs:(j + 1) * bs, :] = jnp.where(goal == spot, 1.0, 0.0).astype(place.dtype)
        return carry

    def fill_far(k, carry):
        m = lax.rem(x * chip_blocks + chip_blocks + k, nblk)
        spot = lax.broadcasted_iota(jnp.int32, (bs, live), 1)
        for q in range(neigh):
            slot = lax.broadcasted_iota(jnp.int32, (bs, 1), 0) + q * bs
            goal = jnp.full((bs, 1), -1, jnp.int32)
            at = 0
            for j in range(neigh):
                b = pair_ref[j, m]
                inside = (slot >= at) & (slot < at + counts_ref[b])
                goal = jnp.where(inside, slot - at + start_ref[b], goal)
                at = at + counts_ref[b]
            place[nblk + k, q * bs:(q + 1) * bs, :] = jnp.where(goal == spot, 1.0, 0.0).astype(place.dtype)
            for down in range(tall):
                inside = (q < width_ref[m]) & (down < tiles_ref[m])
                give_ref[(k * neigh + q) * tall + down] = jnp.where(
                    inside, base_ref[m] + down * width_ref[m] + q, 0
                )
        return carry

    def fill_lift(q, carry):
        spot = lax.broadcasted_iota(jnp.int32, (bs, bs), 0) + q * bs
        slot = lax.broadcasted_iota(jnp.int32, (1, bs), 1)
        for b in range(nblk):
            goal = jnp.where(slot < counts_ref[b], slot + start_ref[b], -1)
            lift[pl.ds(pl.multiple_of(q * bs, bs), bs), b * bs:(b + 1) * bs] = jnp.where(
                goal == spot, 1.0, 0.0
            ).astype(lift.dtype)
        return carry

    def put_wide(m, left, which):
        wide[pl.ds(pl.multiple_of(m * bs, bs), bs), :] = jnp.dot(
            left, place[which], preferred_element_type=jnp.float32
        ).astype(wide.dtype)

    def take_near(i):
        own_copy(0, i).wait()
        core_copy(0, i).wait_recv()

        def put(mm, carry):
            m = x * chip_blocks + mm
            put_wide(m, jnp.concatenate([raw[0, i, mm, j] for j in range(neigh)], axis=1), m)
            return carry

        lax.fori_loop(0, chip_blocks, put, 0)

    def take_far(i):
        for r in range(xs - 1):
            x_copy(xs - 1 - r, i).wait_recv()
            arrived[...] = inbox[r, i]

            def spread(mm, carry):
                for q in range(neigh * tall):
                    stage[mm * neigh * tall + q] = arrived[give_ref[(r * chip_blocks + mm) * neigh * tall + q]]
                close = jnp.concatenate(
                    [stage[pl.ds((mm * neigh + j) * tall, tall)].reshape(bs, bs) for j in range(neigh)], axis=1
                )
                put_wide(x_at(r + 1) * chip_blocks + mm, close, nblk + r * chip_blocks + mm)
                return carry

            lax.fori_loop(0, chip_blocks, spread, 0)

    def take_plain():
        for r in range(xs - 1):
            plain_arrival(r, 0).wait_recv()
            plain_arrival(r, 1).wait_recv()

            def put(mm, carry):
                m = x_at(r + 1) * chip_blocks + mm
                put_wide(m, jnp.concatenate([direct[r, mm, j] for j in range(neigh)], axis=1), m)
                return carry

            lax.fori_loop(0, chip_blocks, put, 0)

    hop(1, 0)
    lax.fori_loop(1, 2, emit, 0)
    lax.fori_loop(0, live // bs, fill_lift, 0)
    def hop_and_emit(h, carry):
        hop(h, carry)
        lax.fori_loop(jnp.minimum(h, per), jnp.minimum(h + 1, per), emit, 0)
        return carry

    lax.fori_loop(2, zs, hop_and_emit, 0)
    lax.fori_loop(0, nblk, fill_place, 0)
    from_y(zs - 1)
    lax.fori_loop(0, (xs - 1) * chip_blocks, fill_far, 0)
    take_near(0)
    take_plain()
    lax.fori_loop(min(zs, per), per, emit, 0)

    def settle(zz, carry):
        for xx in range(xs):
            for yy in range(ys):
                dens_c(xx, zz, yy).wait()
            for e in range(1, ys):
                dens_y(e, xx, zz).wait_send()

            @pl.when((z < zs - 1) & (zz <= z))
            def _():
                dens_z(True, xx, zz).wait_send()

            @pl.when((z > 0) & (zz >= z))
            def _():
                dens_z(False, xx, zz).wait_send()

        return carry

    lax.fori_loop(0, zs, settle, 0)
    for e in range(1, xs):
        dens_x(e).wait_send()

    lane = lax.broadcasted_iota(jnp.int32, (1, bs), 1)
    col_live = jnp.concatenate(
        [jnp.where(lane < counts_ref[b], 1.0, 0.0).astype(jnp.float32) for b in range(nblk)], axis=1
    )

    side = live // 2
    part_cols = min(nbf, 512)

    def fill_near(g, carry):
        at = at_rows(g * group, group)
        for k in range(nbf // part_cols):
            lo = k * part_cols
            found = jnp.dot(lift[at, :], dens[:, lo:lo + part_cols], preferred_element_type=jnp.float32)
            near[at, lo:lo + part_cols] = (found * col_live[:, lo:lo + part_cols]).astype(near.dtype)
        return carry

    def at_rows(first, count):
        return pl.ds(pl.multiple_of(first, 16), count)

    lax.fori_loop(0, live // group, fill_near, 0)

    deep = chip_blocks * bs

    def first_half(first, count):
        at = at_rows(first, count)
        for k in range(nbf // part_cols):
            lo = k * part_cols
            half[at, lo:lo + part_cols] = jnp.dot(
                wide[at, :], near[:, lo:lo + part_cols], preferred_element_type=jnp.float32
            ).astype(half.dtype)

    def second_half(first, count):
        at = at_rows(first, count)
        for lo in range(0, live, part_cols):
            hi = min(lo + part_cols, live)
            total[at, lo:hi] += jnp.dot(half[at, :], wide[:, lo:hi], preferred_element_type=jnp.float32)

    def half_cols(h):
        return slice(h * side, (h + 1) * side)

    def product(g, h):
        at = at_rows(g * group, group)
        total[at, half_cols(h)] += jnp.dot(half[at, :], wide[:, half_cols(h)], preferred_element_type=jnp.float32)

    def one(i, carry):
        def part(xx, carry):
            first_half(xx * deep, deep)
            second_half(xx * deep, deep)
            return carry

        lax.fori_loop(0, xs, part, 0)

        take_near(i + 1)

        @pl.when(i < per - 2)
        def _():
            take_far(i + 1)

        return carry

    lax.fori_loop(0, per - 1, one, 0)

    counter[0] = 0
    ksems = (k_send, k_recv)
    sends = []

    def send_to(src, dst, device):
        cp = remote(src, dst, device, ksems)
        cp.start()
        sends.append(cp)
        return cp

    def part_product(g, q, h):
        at = at_rows(g * group, group)
        qt = at_rows(q * deep, deep)
        qc = pl.ds(pl.multiple_of(q * deep, 128), deep)
        total[at, half_cols(h)] += jnp.dot(
            half[at, qc], wide[qt, half_cols(h)], preferred_element_type=jnp.float32
        )

    def final(e, carry):
        @pl.when(e == 1)
        def _():
            take_far(per - 1)

        def turn(core, carry):
            first_half((x_at(e) * 2 + core) * group, group)

            @pl.when(e == 0)
            def _():
                part_product(x * 2 + core, x, 0)
                part_product(x * 2 + core, x, 1)

            return carry

        lax.fori_loop(0, 2, turn, 0)
        return carry

    lax.fori_loop(0, xs, final, 0)

    def last_product(e, core, h):
        if e:
            product(x_at(e) * 2 + core, h)
        else:
            for f in range(1, xs):
                part_product(x * 2 + core, x_at(f), h)

    left, right = slice(0, side), slice(side, live)

    def y_at(e):
        return lax.rem(y + e, ys)

    core_left, core_right = {}, {}
    for e in list(range(1, xs)) + [0]:
        last_product(e, other, 0)
        last_product(e, other, 1)
        for store, part in ((core_left, left), (core_right, right)):
            store[e] = send_to(
                total.at[at_rows((x_at(e) * 2 + other) * group, group), part],
                from_core.at[e * group:(e + 1) * group, part],
                sibling,
            )

    def core_sum(e, row, count, part):
        return (
            total[at_rows((x_at(e) * 2 + c) * group + row, count), part]
            + from_core[at_rows(e * group + row, count), part]
        )

    zr = zs * rows
    left_x = {}
    for e in range(1, xs):
        last_product(e, c, 0)
        core_left[e].wait_recv()
        for f in list(range(1, ys)) + [0]:
            lo = (e - 1) * group + f * zr
            def pour(zz, carry):
                send[at_rows(lo + zz * rows, rows), left] = core_sum(
                    e, (zz * ys + y_at(f)) * rows, rows, left
                ).astype(send.dtype)
                return carry

            lax.fori_loop(0, zs, pour, 0)
            left_x[e, f] = send_to(
                send.at[lo:lo + zr, left], first_x.at[lo:lo + zr, :], (x_at(e) * 2 + c, u)
            )
    right_y = {}
    for e in list(range(1, xs)) + [0]:
        last_product(e, c, 1)
        core_right[e].wait_recv()
        for f in range(1, ys):
            lo = ((f - 1) * xs + e) * zr
            to = (f - 1) * xs * zr + x_at(e) * zr
            def pour(zz, carry):
                send[at_rows(lo + zz * rows, rows), right] = core_sum(
                    e, (zz * ys + y_at(f)) * rows, rows, right
                ).astype(send.dtype)
                return carry

            lax.fori_loop(0, zs, pour, 0)
            right_y[f, e] = send_to(
                send.at[lo:lo + zr, right], second_y.at[at_rows(to, zr), :], (t, y_peer(f))
            )
    last_product(0, c, 0)
    core_left[0].wait_recv()

    def left_after_x(zz, f):
        value = core_sum(0, (zz * ys + y_at(f)) * rows, rows, left)
        for e in range(xs - 1):
            row = e * group + f * zr + zz * rows
            value = value + first_x[at_rows(row, rows), :].astype(jnp.float32)
        return value

    stage = max((xs - 1) * group, (ys - 1) * xs * zr)
    left_y = []
    for f in range(1, ys):
        lo = stage + (f - 1) * zr
        for e in range(1, xs):
            left_x[e, f].wait_recv()
        def pour(zz, carry):
            send[at_rows(lo + zz * rows, rows), left] = left_after_x(zz, f).astype(send.dtype)
            return carry

        lax.fori_loop(0, zs, pour, 0)
        left_y.append(send_to(
            send.at[lo:lo + zr, left], first_y.at[(f - 1) * zr:f * zr, :], (t, y_peer(f))
        ))

    def right_after_y(e, zz):
        value = core_sum(e, (zz * ys + y) * rows, rows, right)
        for f in range(ys - 1):
            row = f * xs * zr + x_at(e) * zr + zz * rows
            value = value + second_y[at_rows(row, rows), :].astype(jnp.float32)
        return value

    right_x = []
    for e in range(1, xs):
        lo = stage + (e - 1) * zr
        for f in range(1, ys):
            right_y[f, e].wait_recv()
        def pour(zz, carry):
            send[at_rows(lo + zz * rows, rows), right] = right_after_y(e, zz).astype(send.dtype)
            return carry

        lax.fori_loop(0, zs, pour, 0)
        right_x.append(send_to(
            send.at[lo:lo + zr, right], second_x.at[(e - 1) * zr:e * zr, :], (x_at(e) * 2 + c, u)
        ))

    def left_after_y(zz):
        value = left_after_x(zz, 0)
        for f in range(ys - 1):
            value = value + first_y[at_rows(f * zr + zz * rows, rows), :].astype(jnp.float32)
        return value

    def right_after_x(zz):
        value = right_after_y(0, zz)
        for e in range(xs - 1):
            value = value + second_x[at_rows(e * zr + zz * rows, rows), :].astype(jnp.float32)
        return value

    stage = stage + max(xs - 1, ys - 1) * zr
    ends = []
    for waits, after, into, part in (
        (left_y, left_after_y, first_z, left), (right_x, right_after_x, second_z, right)
    ):
        for cp in waits:
            cp.wait_recv()
        if part == right:
            for f in range(1, ys):
                right_y[f, 0].wait_recv()
        else:
            for e in range(1, xs):
                left_x[e, 0].wait_recv()
        arrivals = []
        for e in range(1, zs):
            lo = stage + (e - 1) * rows
            send[lo:lo + rows, part] = after(lax.rem(z + e, zs)).astype(send.dtype)
            arrivals.append(send_to(
                send.at[lo:lo + rows, part], into.at[(e - 1) * rows:e * rows, :], (t, z_peer(e))
            ))
        ends.append((arrivals, after, into, part))
    block = mine // bs
    slot = lax.broadcasted_iota(jnp.int32, (rows, 1), 0) + mine % bs
    row_live = jnp.where(slot < counts_ref[block], 1.0, 0.0).astype(jnp.float32)
    for arrivals, after, into, part in ends:
        value = after(z)
        for e in range(zs - 1):
            arrivals[e].wait_recv()
            value = value + into[e * rows:(e + 1) * rows, :].astype(jnp.float32)
        for k in range(3):
            bits = value.astype(cut.dtype)
            cut[k * rows:(k + 1) * rows, part] = bits
            value = value - bits.astype(jnp.float32)
    whole = jnp.dot(cut[...], lift[...], preferred_element_type=jnp.float32)
    whole = whole[:rows] + whole[rows:2 * rows] + whole[2 * rows:]
    out_ref[...] = whole * row_live
    for cp in sends:
        cp.wait_send()

    def finish(i, carry):
        core_copy(0, i).wait_send()

        @pl.when(i > 0)
        def _():
            for e in range(1, xs):
                core_copy(e, i).wait_send()
                x_copy(e, i).wait_send()

        return carry

    lax.fori_loop(0, per, finish, 0)
    for e in range(1, xs):
        plain_copy(e, 0).wait_send()
        plain_copy(e, 1).wait_send()


def packed_caps(chip_blocks, neigh, bs):
    full = chip_blocks * neigh * (bs // 16)
    return [full * k // 32 // 4 * 4 for k in (23, 25, 28)] + [full]


def packed_scratch(cap, atoms, aux, xs, ys, zs, per, nblk, neigh, bs, rows):
    nbf, chip_blocks, group = nblk * bs, nblk // xs, aux * rows
    live = nbf * 3 // 4
    side, zr, span, tall = live // 2, zs * rows, neigh * bs, bs // 16
    n_k = 2 * (xs + (xs - 1) + (ys - 1) + (zs - 1)) + 2 * (xs - 1) * (ys - 1)
    send_rows = max((xs - 1) * group, (ys - 1) * xs * zr) + max(xs - 1, ys - 1) * zr + zr
    vmem, smem, dma = pltpu.VMEM, pltpu.SMEM, pltpu.SemaphoreType.DMA
    bf16, f32 = jnp.bfloat16, jnp.float32
    far = max(xs - 1, 1)
    return [
        smem((neigh, nblk), jnp.int32),
        smem((nblk,), jnp.int32),
        smem((nblk,), jnp.int32),
        smem((nblk,), jnp.int32),
        smem((nblk,), jnp.int32),
        smem((nblk,), jnp.int32),
        smem((cap,), jnp.int32),
        smem((far * chip_blocks * neigh * tall,), jnp.int32),
        vmem((nbf, nbf), bf16),
        vmem((xs, per, chip_blocks, neigh, bs, bs), bf16),
        vmem((far, chip_blocks, neigh, bs, bs), bf16),
        vmem((far, per, cap, 16, bs), bf16),
        vmem((far, per, cap, 16, bs), bf16),
        vmem((chip_blocks * neigh * tall, 16, bs), bf16),
        vmem((cap, 16, bs), bf16),
        vmem((chip_blocks, span, span), bf16),
        vmem((nblk + far * chip_blocks, span, live), bf16),
        vmem((live, nbf), bf16),
        vmem((live, nbf), bf16),
        vmem((nbf, live), bf16),
        vmem((nbf, nbf), bf16),
        vmem((send_rows, live), bf16),
        vmem((nbf, live), f32),
        vmem((xs * group, live), f32),
        vmem((far * group, side), bf16),
        vmem((max(ys - 1, 1) * zr, side), bf16),
        vmem((max(zs - 1, 1) * rows, side), bf16),
        vmem((max(ys - 1, 1) * xs * zr, side), bf16),
        vmem((far * zr, side), bf16),
        vmem((max(zs - 1, 1) * rows, side), bf16),
        vmem((3 * rows, live), bf16),
        dma((xs, per)),
        dma,
        dma,
        dma,
        dma((xs, per)),
        dma((xs, per)),
        dma((far, 2)),
        dma((far, 2)),
        dma((far, per)),
        dma((far, per)),
        dma((far,)),
        dma((far,)),
        dma((2, zs, xs)),
        dma((zs, xs)),
        dma((zs, xs, max(ys - 1, 1))),
        dma((zs, xs, max(ys - 1, 1))),
        dma((zs, ys, xs)),
        dma((zs, ys, xs)),
        dma((n_k,)),
        dma((n_k,)),
    ]


VMEM_BYTES = 67043328


def packed_call(which, cap, sizes, three_index, density, pair_blocks, basis_counts):
    atoms, aux, xs, ys, zs = sizes[:5]
    rows, nbf = density.shape
    anywhere = pl.BlockSpec(memory_space=pl.ANY)
    return pl.pallas_call(
        functools.partial(packed_kernel, cap, atoms, aux, xs, ys, zs),
        out_shape=jax.ShapeDtypeStruct((rows, nbf), jnp.float32),
        in_specs=[anywhere] * 4,
        out_specs=pl.BlockSpec(memory_space=pltpu.VMEM),
        scratch_shapes=packed_scratch(cap, *sizes),
        compiler_params=pltpu.CompilerParams(
            collective_id=which, has_side_effects=True, vmem_limit_bytes=VMEM_BYTES
        ),
    )(pair_blocks.T, basis_counts, three_index, density)


def per_device(atoms, aux, three_index, density, pair_blocks, basis_counts):
    aux_here, own_blocks, neigh, bs, _ = three_index.shape
    rows, nbf = density.shape
    nblk = nbf // bs
    xs = atoms // 2
    ys = xs if aux % xs == 0 else 1
    zs = aux // ys
    per = aux_here // atoms
    sizes = (atoms, aux, xs, ys, zs, per, nblk, neigh, bs, rows)
    caps = packed_caps(nblk // xs, neigh, bs)
    need = sum(
        math.prod(ref.shape) * jnp.dtype(ref.dtype).itemsize
        for ref in packed_scratch(caps[-1], *sizes) if getattr(ref, 'memory_space', None) == pltpu.VMEM
    )
    if per < 2 or nbf * 3 // 4 % (aux * rows) or nbf * 3 % (8 * bs) or need + 2 * rows * nbf * 4 > VMEM_BYTES - 2**21:
        return plain_device(atoms, aux, three_index, density, pair_blocks, basis_counts)
    hit = pair_blocks[:, :, None] == jnp.arange(nblk)[None, None, :]
    lanes = jnp.sum(jnp.where(hit, basis_counts[None, None, :], 0), axis=(1, 2))
    width = sum((lanes > k * bs).astype(jnp.int32) for k in range(neigh))
    tiles = ((basis_counts + 15) >> 4) * width
    chip = functools.reduce(jnp.maximum, [jnp.sum(jnp.where(jnp.arange(nblk) // (nblk // xs) == k, tiles, 0)) for k in range(xs)])
    choice = sum((chip > cap).astype(jnp.int32) for cap in caps[:-1])
    branches = [functools.partial(packed_call, k, cap, sizes) for k, cap in enumerate(caps)]
    return lax.switch(choice, branches, three_index, density, pair_blocks, basis_counts)


def solution(mesh):
    in_specs = (P("aux", "atom", None, None, None), P(("atom", "aux"), None), P(), P())
    out_specs = P(("atom", "aux"), None)
    return jax.shard_map(
        functools.partial(per_device, mesh.shape["atom"], mesh.shape["aux"]),
        mesh=mesh, in_specs=in_specs, out_specs=out_specs, check_vma=False,
    )
```
